512 devices in a mesh: section: 2 (over z_lo), wrow: 16 (over y, core), wcol: 16 (over x, z_hi).
Axes of the slice: x: 4, y: 8, z: 8 (z_hi: 4, z_lo: 2; z = z_hi * 2 + z_lo), core: 2. Of those that a mesh axis runs over, the one named last changes fastest.
Arguments:
- states: bfloat16 [2, 256, 256, 1536], P(None, 'wrow', 'wcol'), may hold values from -6 to 6
- timesteps: int32 [2], replicated, may hold values from 0 to 999, as said below
- shifts: int32 [2, 2], P('section'), may hold values from 1 to 4
- qkv_weight: bfloat16 [2, 1536, 2304], P('section', None, 'wcol'), may hold values from -0.15625 to 0.15625
- out_weight: bfloat16 [2, 768, 1536], P('section', None, 'wcol'), may hold values from -0.21875 to 0.21875
- mod_weight: bfloat16 [2, 256, 4608], P('section', None, 'wcol'), may hold values from -0.375 to 0.375
Outputs:
- layer_states: bfloat16 [2, 2, 256, 256, 1536], P('section', None, 'wrow', 'wcol')
The draws below stay inside these ranges and needn't reach their ends.
Inputs may be any that keep to these rules, and one draw needn't show every extreme that they name: The 2 timesteps are distinct.
All inputs are finite; a program needn't handle non-finite values.
Results may differ from the reference program's by a relative error of at most 0.0053.
Values may be sent and summed in bfloat16 or wider, within the bound.
A program may use at most 128 MiB of HBM per device.

```python
import math
import jax
import jax.numpy as jnp
from jax import lax

D = 1536
HEADS = 6
HD = 128
TEMB = 256
WIN = 8
MB = 2
HH = 768
QKV = 2304
NH = 256
NW = 256
SECTIONS = 2
N_SECTION = 2


def draw_timesteps(key, part):
    first_key, second_key = jax.random.split(jax.random.fold_in(key, 7129))
    largest_step = 999 // max(MB - 1, 1)
    step_value = jax.random.randint(first_key, (), 1, largest_step + 1, dtype=jnp.int32)
    counter = jnp.arange(MB, dtype=jnp.int32)
    values = 999 - counter * step_value
    offset = jax.random.randint(second_key, (), 0, MB, dtype=jnp.int32)
    return jnp.roll(values, offset).astype(jnp.int32)


def plant(values, key, least, top_value):
    longest = values.shape.index(max(values.shape))
    spots = []
    for shift in (0, 1):
        where = [jax.random.randint(jax.random.fold_in(key, axis), (), 0, length) for axis, length in enumerate(values.shape)]
        where[longest] = (where[longest] + shift) % values.shape[longest]
        spots.append(tuple(where))
    return values.at[spots[0]].set(least).at[spots[1]].set(top_value)


def steps_of(key, extent, pieces, smallest, largest):
    gain, own = 1.0, jax.random.fold_in(key, 6)
    for position, blocks in pieces:
        steps = jnp.exp(jax.random.uniform(jax.random.fold_in(own, position), (blocks,), jnp.float32, smallest / len(pieces), largest / len(pieces)))
        gain = gain * jnp.repeat(steps, extent[position] // blocks).reshape([-1 if axis == position else 1 for axis in range(len(extent))])
    return gain


def normal_values(stream_key, dims, width, most, shards=(), held_as=jnp.bfloat16):
    values = width * jax.random.normal(stream_key, dims, jnp.float32)
    if shards:
        values = values * steps_of(stream_key, dims, shards, -0.22, 0.18)
    return jnp.clip(values, -most, most).astype(held_as)


def setup_inputs(seed: int = 0) -> dict:
    key_list = jax.random.split(jax.random.key(seed), 7)
    states = normal_values(key_list[0], (MB, NH, NW, D), 1.0, 6.0, ((1, 16), (2, 16)))
    timesteps = draw_timesteps(jax.random.fold_in(key_list[6], 71), 0)
    shifts = plant(jax.random.randint(key_list[2], (SECTIONS, 2), 1, WIN // 2 + 1), jax.random.fold_in(key_list[2], 1), 1, (WIN // 2 + 1) - 1).astype(jnp.int32)
    qkv_weight = normal_values(key_list[3], (SECTIONS, D, QKV), D ** -0.5, 0.15625, ((0, 2), (2, 16)))
    out_weight = normal_values(key_list[4], (SECTIONS, HH, D), HH ** -0.5, 0.21875, ((0, 2), (2, 16)))
    mod_weight = normal_values(key_list[5], (SECTIONS, TEMB, 3 * D), TEMB ** -0.5, 0.375, ((0, 2), (2, 16)))
    return dict(states=states, timesteps=timesteps, shifts=shifts, qkv_weight=qkv_weight, out_weight=out_weight, mod_weight=mod_weight)


epsilon = 1e-06

def sinusoid(moments, entries):
    half_count = entries // 2
    frequency = jnp.exp(-math.log(10000.0) * jnp.arange(half_count, dtype=jnp.float32) / half_count)
    angles = moments.astype(jnp.float32)[:, None] * frequency[None, :]
    return jnp.concatenate([jnp.cos(angles), jnp.sin(angles)], axis=1)

def rounded(number):
    return lax.optimization_barrier(number.astype(jnp.bfloat16)).astype(jnp.float32)

def layer_norm(region):
    values = region.astype(jnp.float32)
    center = values - lax.optimization_barrier(jnp.mean(values, axis=-1, keepdims=True))
    spread = lax.optimization_barrier(jnp.mean(center * center, axis=-1, keepdims=True))
    return center * lax.rsqrt(spread + epsilon)

def window_attention(triples):
    tile_rows, tile_cols, feature_width = triples.shape
    windowed = triples.reshape(tile_rows // WIN, WIN, tile_cols // WIN, WIN, 3, HEADS, HD)
    windowed = windowed.transpose(4, 0, 2, 5, 1, 3, 6).reshape(3, tile_rows // WIN * (tile_cols // WIN), HEADS, WIN * WIN, HD)
    scores = jnp.einsum('nhqd,nhkd->nhqk', windowed[0].astype(jnp.float32), windowed[1].astype(jnp.float32)) * HD ** (-0.5)
    weights = jnp.exp(scores)
    probabilities = (weights / lax.optimization_barrier(jnp.sum(weights, axis=-1, keepdims=True))).astype(jnp.bfloat16)
    attended = jnp.einsum('nhqk,nhkd->nhqd', probabilities.astype(jnp.float32), windowed[2].astype(jnp.float32)).astype(jnp.bfloat16)
    attended = attended.reshape(tile_rows // WIN, tile_cols // WIN, HEADS, WIN, WIN, HD).transpose(0, 3, 1, 4, 2, 5)
    return attended.reshape(tile_rows, tile_cols, HEADS * HD)

def by_bands(function, *arrays):
    stacked = tuple((member.reshape((member.shape[0] // WIN, WIN) + member.shape[1:]) for member in arrays))
    result = lax.map(lambda members: function(*members), stacked)
    return result.reshape((-1,) + result.shape[2:])

def shifted_layer(inputs, modulation, shift_pair, qkv_matrix, out_matrix):
    mod_shift = modulation[:D]
    mod_scale = modulation[D:2 * D]
    mod_gate = modulation[2 * D:]

    def normalize(stripe):
        return (layer_norm(stripe) * (1.0 + mod_scale) + mod_shift).astype(jnp.bfloat16)
    normed = by_bands(normalize, inputs)
    rolled = jnp.roll(normed, (-shift_pair[0], -shift_pair[1]), axis=(0, 1))

    def attend(stripe):
        tile_rows, tile_cols, feature_width = stripe.shape
        triples = jnp.dot(stripe.reshape(tile_rows * tile_cols, feature_width), qkv_matrix, preferred_element_type=jnp.float32)
        return window_attention(triples.astype(jnp.bfloat16).reshape(tile_rows, tile_cols, -1))
    attended = by_bands(attend, rolled)
    restored = jnp.roll(attended, (shift_pair[0], shift_pair[1]), axis=(0, 1))

    def finish(stripe, residual):
        tile_rows, tile_cols, feature_width = stripe.shape
        projection = jnp.dot(stripe.reshape(tile_rows * tile_cols, feature_width), out_matrix, preferred_element_type=jnp.float32)
        projection = rounded(projection).reshape(tile_rows, tile_cols, -1)
        return (residual.astype(jnp.float32) + mod_gate * projection).astype(jnp.bfloat16)
    return by_bands(finish, restored, inputs)

def reference(states, timesteps, shifts, qkv_weight, out_weight, mod_weight):
    embedding = jax.nn.silu(sinusoid(timesteps, TEMB)).astype(jnp.bfloat16)
    current = states
    results = []
    for section_index in range(N_SECTION):
        modulations = rounded(jnp.dot(embedding, mod_weight[section_index], preferred_element_type=jnp.float32))
        current = jnp.stack([shifted_layer(current[member], modulations[member], shifts[section_index], qkv_weight[section_index], out_weight[section_index]) for member in range(MB)])
        results.append(current)
    return jnp.stack(results)
```

```python
import functools
import math

import jax
import jax.numpy as jnp
from jax import lax
from jax.experimental import pallas as pl
from jax.experimental.pallas import tpu as pltpu
from jax.sharding import PartitionSpec as P

HEADS = 6
HD = 128
TEMB = 256
WIN = 8
MB = 2
MESH = pl.DeviceIdType.MESH
UNIT = 48


epsilon = 1e-06


def passed_along(shard, axis, by):
    devices = lax.axis_size(axis)
    return lax.ppermute(shard, axis, [(i, (i + by) % devices) for i in range(devices)])


def from_behind(shard, axis, by):
    devices = lax.axis_size(axis)
    pairs = [(i, i + by) for i in range(devices) if 0 <= i + by < devices]
    return lax.ppermute(shard, axis, pairs)


def sinusoid(moments, entries):
    half_count = entries // 2
    frequency = jnp.exp(-math.log(10000.0) * jnp.arange(half_count, dtype=jnp.float32) / half_count)
    angles = moments.astype(jnp.float32)[:, None] * frequency[None, :]
    return jnp.concatenate([jnp.cos(angles), jnp.sin(angles)], axis=1)


def rounded(number):
    return lax.optimization_barrier(number.astype(jnp.bfloat16)).astype(jnp.float32)


def layer_norm(region):
    values = region.astype(jnp.float32)
    center = values - jnp.mean(values, axis=-1, keepdims=True)
    spread = jnp.mean(center * center, axis=-1, keepdims=True)
    return center * lax.rsqrt(spread + epsilon)


def window_attention(triples):
    tile_rows, tile_cols, feature_width = triples.shape
    windowed = triples.reshape(tile_rows // WIN, WIN, tile_cols // WIN, WIN, 3, HEADS, HD)
    windowed = windowed.transpose(4, 0, 2, 5, 1, 3, 6).reshape(
        3, tile_rows // WIN * (tile_cols // WIN), HEADS, WIN * WIN, HD
    )
    scores = jnp.einsum(
        "nhqd,nhkd->nhqk", windowed[0], windowed[1], preferred_element_type=jnp.float32
    ) * HD ** (-0.5)
    weights = jnp.exp(scores)
    probabilities = (weights / jnp.sum(weights, axis=-1, keepdims=True)).astype(jnp.bfloat16)
    attended = jnp.einsum(
        "nhqk,nhkd->nhqd", probabilities, windowed[2], preferred_element_type=jnp.float32
    ).astype(jnp.bfloat16)
    attended = attended.reshape(tile_rows // WIN, tile_cols // WIN, HEADS, WIN, WIN, HD).transpose(
        0, 3, 1, 4, 2, 5
    )
    return attended.reshape(tile_rows, tile_cols, HEADS * HD)


def project(region, matrix_t):
    tile_rows, tile_cols, feature_width = region.shape
    product = lax.dot_general(
        region.reshape(tile_rows * tile_cols, feature_width),
        matrix_t,
        (((1,), (1,)), ((), ())),
        preferred_element_type=jnp.float32,
    )
    return product.reshape(tile_rows, tile_cols, -1)


def splice(region, border, amount, direction, margin, axis_index):
    if direction > 0:
        longer = jnp.concatenate([region, border], axis=axis_index)
        offset = amount
    else:
        longer = jnp.concatenate([border, region], axis=axis_index)
        offset = margin - amount
    return lax.dynamic_slice_in_dim(longer, offset, region.shape[axis_index], axis_index)


def wrap_rim(region, row_shift, col_shift, direction):
    margin = WIN // 2
    if direction > 0:
        border = region[:margin]
    else:
        border = region[region.shape[0] - margin :]
    border = passed_along(border, "wrow", -direction)
    region = splice(region, border, row_shift, direction, margin, 0)
    if direction > 0:
        border = region[:, :margin]
    else:
        border = region[:, region.shape[1] - margin :]
    border = passed_along(border, "wcol", -direction)
    return splice(region, border, col_shift, direction, margin, 1)


def shifted_layer(inputs, modulation, row_shift, col_shift, qkv_t, out_t):
    feature_width = inputs.shape[-1]
    mod_shift = modulation[:feature_width]
    mod_scale = modulation[feature_width : 2 * feature_width]
    mod_gate = modulation[2 * feature_width :]
    normed = (layer_norm(inputs) * (1.0 + mod_scale) + mod_shift).astype(jnp.bfloat16)
    triples = project(normed, qkv_t).astype(jnp.bfloat16)
    triples = wrap_rim(triples, row_shift, col_shift, 1)
    attended = window_attention(triples)
    restored = wrap_rim(attended, row_shift, col_shift, -1)
    projection = rounded(project(restored, out_t))
    return (inputs.astype(jnp.float32) + mod_gate * projection).astype(jnp.bfloat16)


def unit_row(w, q):
    last = q // 3
    return (144 * w + UNIT * q) * (1 - last) + (2304 + UNIT * w) * last


ORDER = (
    (0, -1), (0, 1), (-1, 0), (1, 0), (0, 2), (-1, -1), (1, -1), (-1, 1), (1, 1),
    (-1, 2), (1, 2), (2, 0), (2, -1), (2, 1), (2, 2),
)


def place():
    row, col = lax.axis_index("wrow"), lax.axis_index("wcol")
    return row, col, row // 2, row % 2, col // 4, col % 4


def gather_weights(comb, weights, sem_own, sem_send, sem_recv, sem_half):
    row, col, y, core, x, z = place()
    q = (y % 2) * 2 + core
    counter = [0]
    sends = []

    def unit(w, quarter, first=0, count=UNIT):
        start = pl.multiple_of(unit_row(w, quarter) + first, 16)
        return weights.at[pl.ds(start, count), :]

    def copy(w, quarter, target, slot, first=0, count=UNIT, recv=None):
        part = unit(w, quarter, first, count)
        return pltpu.make_async_remote_copy(
            src_ref=part,
            dst_ref=part,
            send_sem=sem_send.at[slot],
            recv_sem=sem_recv.at[w * 4 + quarter] if recv is None else recv,
            device_id=target,
            device_id_type=MESH,
        )

    def send(w, quarter, target, **kw):
        c = copy(w, quarter, target, counter[0], **kw)
        counter[0] += 1
        c.start()
        sends.append(c)

    def arrived(w, quarter, **kw):
        copy(w, quarter, {"wrow": row}, 0, **kw).wait_recv()

    def at_col(dx, dz):
        return {"wcol": ((x + dx + 4) % 4) * 4 + (z + dz + 4) % 4}

    partner = {"wrow": y * 2 + 1 - core}

    def number(dx, dz):
        return ((x + dx + 4) % 4) * 4 + (z + dz + 4) % 4

    def to_row(w):
        up = (w // 4 + w % 4) % 2
        return {"wrow": ((y + 7 + 2 * up) % 8) * 2 + core}

    own = []
    for quarter in range(4):
        c = pltpu.make_async_copy(
            comb.at[pl.ds(UNIT * quarter, UNIT), :], unit(col, quarter), sem_own.at[quarter]
        )
        c.start()
        own.append(c)

    def begin():
        for c in own:
            c.wait()
        for d in ((0, 1), (0, -1), (1, 0), (-1, 0)):
            send(col, q, at_col(*d))

    def plane():
        for dx, dz in ORDER:
            w = number(dx, dz)
            if (dx, dz) == (0, 2):
                arrived(w, q, first=0, count=32, recv=sem_half.at[0])
                arrived(w, q, first=32, count=16, recv=sem_half.at[1])
            else:
                arrived(w, q)
            if dx == 0:
                send(w, q, at_col(1, 0))
                send(w, q, at_col(-1, 0))
                if dz == -1:
                    send(w, q, at_col(0, 1), first=0, count=32, recv=sem_half.at[0])
                if dz == 1:
                    send(w, q, at_col(0, -1), first=32, count=16, recv=sem_half.at[1])
            if dx == -1 and dz in (0, -1):
                send(w, q, at_col(1, 0))
            if dx == 1 and dz in (1, 2):
                send(w, q, at_col(-1, 0))
            send(w, q, to_row(w))
            send(w, q, partner)

    def rows():
        qy = ((y + 1) % 2) * 2 + core
        for d in ORDER:
            arrived(number(*d), qy)
            send(number(*d), qy, partner)

    def sides():
        for d in ORDER:
            arrived(number(*d), (y % 2) * 2 + 1 - core)
        for d in ORDER:
            arrived(number(*d), ((y + 1) % 2) * 2 + 1 - core)

    def finish():
        for c in sends:
            c.wait_send()

    return begin, plane, rows, sides, finish


def gather_kernel(
    comb, mod_own, w_out, mods, weights, sem_own, sem_send, sem_recv, sem_half, sem_ms, sem_mr, sem_o
):
    row, col, y, core, x, z = place()
    begin, plane, rows, sides, finish = gather_weights(
        comb, weights, sem_own, sem_send, sem_recv, sem_half
    )
    barrier = pltpu.get_barrier_semaphore()
    peers = [{"wcol": (col + k) % 16} for k in range(1, 16)]
    near = [
        {"wrow": y * 2 + 1 - core},
        {"wrow": ((y + 1) % 8) * 2 + core},
        {"wrow": ((y + 7) % 8) * 2 + core},
    ]
    for peer in peers + near:
        pl.semaphore_signal(barrier, inc=1, device_id=peer, device_id_type=MESH)
    pl.semaphore_wait(barrier, 18)
    begin()
    mods[pl.ds(col, 1)] = mod_own[...][None]
    msends = []
    for k in range(1, 16):
        c = pltpu.make_async_remote_copy(
            src_ref=mod_own,
            dst_ref=mods.at[col],
            send_sem=sem_ms.at[k],
            recv_sem=sem_mr.at[col],
            device_id=peers[k - 1],
            device_id_type=MESH,
        )
        c.start()
        msends.append(c)
    plane()
    rows()
    sides()
    for k in range(1, 16):
        other = (col + k) % 16
        pltpu.make_async_remote_copy(
            src_ref=mod_own,
            dst_ref=mods.at[other],
            send_sem=sem_ms.at[k],
            recv_sem=sem_mr.at[other],
            device_id=peers[k - 1],
            device_id_type=MESH,
        ).wait_recv()
    out = pltpu.make_async_copy(weights, w_out, sem_o)
    out.start()
    finish()
    for c in msends:
        c.wait_send()
    out.wait()


def gather(comb, mod_own):
    dma = pltpu.SemaphoreType.DMA
    return pl.pallas_call(
        gather_kernel,
        out_shape=(
            jax.ShapeDtypeStruct((3072, 1536), jnp.bfloat16),
            jax.ShapeDtypeStruct((16, 24, 128), jnp.float32),
        ),
        in_specs=[pl.BlockSpec(memory_space=pl.ANY), pl.BlockSpec(memory_space=pltpu.VMEM)],
        out_specs=(pl.BlockSpec(memory_space=pl.ANY), pl.BlockSpec(memory_space=pltpu.VMEM)),
        scratch_shapes=[
            pltpu.VMEM((3072, 1536), jnp.bfloat16),
            dma((4,)),
            dma((68,)),
            dma((64,)),
            dma((2,)),
            dma((16,)),
            dma((16,)),
            dma,
        ],
        compiler_params=pltpu.CompilerParams(
            collective_id=0, has_side_effects=True, vmem_limit_bytes=48 << 20
        ),
        name="gather",
    )(comb, mod_own)


def packed_modulation(mod_part):
    pieces = mod_part.astype(jnp.float32).reshape(MB * 9, 32)
    return jnp.pad(jnp.tile(pieces, (1, 4)), ((0, 6), (0, 0)))


def per_device(states, timesteps, shifts, qkv_weight, out_weight, mod_weight):
    embedding = jax.nn.silu(sinusoid(timesteps, TEMB)).astype(jnp.bfloat16)
    mod_part = jnp.dot(embedding, mod_weight[0], preferred_element_type=jnp.float32).astype(
        jnp.bfloat16
    )
    out_rows = out_weight[0].T
    comb = jnp.concatenate(
        [qkv_weight[0].T, jnp.concatenate([out_rows[:UNIT], out_rows[UNIT:]], axis=1)], axis=0
    )
    weights, mods = gather(comb, packed_modulation(mod_part))
    qkv_full = weights[:2304]
    out_full = weights[2304:].reshape(16, UNIT, 2, 768).transpose(0, 2, 1, 3).reshape(1536, 768)
    modulations = mods[:, :18, :32].reshape(16, MB, 9 * 32).transpose(1, 0, 2).reshape(MB, -1)
    section_index = lax.axis_index("section")
    moments = MB + lax.axis_size("section") - 1
    row_shift = shifts[0, 0]
    col_shift = shifts[0, 1]
    incoming = jnp.zeros_like(states[0])
    results = jnp.zeros_like(states)
    for moment in range(moments):
        member = moment - section_index
        batch_slot = jnp.clip(member, 0, MB - 1)
        block_input = jnp.where(section_index == 0, states[min(moment, MB - 1)], incoming)
        modulation = lax.dynamic_index_in_dim(modulations, batch_slot, 0, keepdims=False)
        outgoing = shifted_layer(block_input, modulation, row_shift, col_shift, qkv_full, out_full)
        active = (member >= 0) & (member < MB)
        updated = lax.dynamic_update_index_in_dim(results, outgoing, batch_slot, 0)
        results = jnp.where(active, updated, results)
        if moment + 1 < moments:
            incoming = from_behind(outgoing, "section", 1)
    return results[None]


def solution(mesh):
    in_specs = (
        P(None, "wrow", "wcol", None),
        P(),
        P("section", None),
        P("section", None, "wcol"),
        P("section", None, "wcol"),
        P("section", None, "wcol"),
    )
    out_specs = P("section", None, "wrow", "wcol", None)
    return jax.shard_map(
        per_device, mesh=mesh, in_specs=in_specs, out_specs=out_specs, check_vma=False
    )
```

```python
import math

import jax
import jax.numpy as jnp
from jax import lax
from jax.experimental import pallas as pl
from jax.experimental.pallas import tpu as pltpu
from jax.sharding import PartitionSpec as P

HEADS = 6
HD = 128
TEMB = 256
MB = 2
D = 1536
MESH = pl.DeviceIdType.MESH
UNIT = 48
EPSILON = 1e-06
BF16 = jnp.bfloat16
F32 = jnp.float32


def sinusoid(moments, entries):
    half_count = entries // 2
    frequency = jnp.exp(-math.log(10000.0) * jnp.arange(half_count, dtype=jnp.float32) / half_count)
    angles = moments.astype(jnp.float32)[:, None] * frequency[None, :]
    return jnp.concatenate([jnp.cos(angles), jnp.sin(angles)], axis=1)


def unit_row(w, q):
    last = q // 3
    return (144 * w + UNIT * q) * (1 - last) + (2304 + UNIT * w) * last


ORDER = (
    (0, -1), (0, 1), (-1, 0), (1, 0), (0, 2), (-1, -1), (1, -1), (-1, 1), (1, 1),
    (-1, 2), (1, 2), (2, 0), (2, -1), (2, 1), (2, 2),
)


def place():
    row, col = lax.axis_index("wrow"), lax.axis_index("wcol")
    return row, col, row // 2, row % 2, col // 4, col % 4


def gather_weights(comb, weights, sem_own, sem_send, sem_recv, sem_half):
    row, col, y, core, x, z = place()
    q = (y % 2) * 2 + core
    counter = [0]
    sends = []

    def unit(w, quarter, first=0, count=UNIT):
        start = pl.multiple_of(unit_row(w, quarter) + first, 16)
        return weights.at[pl.ds(start, count), :]

    def copy(w, quarter, target, slot, first=0, count=UNIT, recv=None):
        part = unit(w, quarter, first, count)
        return pltpu.make_async_remote_copy(
            src_ref=part,
            dst_ref=part,
            send_sem=sem_send.at[slot],
            recv_sem=sem_recv.at[w * 4 + quarter] if recv is None else recv,
            device_id=target,
            device_id_type=MESH,
        )

    def send(w, quarter, target, **kw):
        c = copy(w, quarter, target, counter[0], **kw)
        counter[0] += 1
        c.start()
        sends.append(c)

    def arrived(w, quarter, **kw):
        copy(w, quarter, {"wrow": row}, 0, **kw).wait_recv()

    def at_col(dx, dz):
        return {"wcol": ((x + dx + 4) % 4) * 4 + (z + dz + 4) % 4}

    partner = {"wrow": y * 2 + 1 - core}

    def number(dx, dz):
        return ((x + dx + 4) % 4) * 4 + (z + dz + 4) % 4

    def to_row(w):
        up = (w // 4 + w % 4) % 2
        return {"wrow": ((y + 7 + 2 * up) % 8) * 2 + core}

    own = []
    for quarter in range(4):
        c = pltpu.make_async_copy(
            comb.at[pl.ds(UNIT * quarter, UNIT), :], unit(col, quarter), sem_own.at[quarter]
        )
        c.start()
        own.append(c)

    def begin():
        for c in own:
            c.wait()
        for d in ((0, 1), (0, -1), (1, 0), (-1, 0)):
            send(col, q, at_col(*d))

    def plane():
        for dx, dz in ORDER:
            w = number(dx, dz)
            if (dx, dz) == (0, 2):
                arrived(w, q, first=0, count=32, recv=sem_half.at[0])
                arrived(w, q, first=32, count=16, recv=sem_half.at[1])
            else:
                arrived(w, q)
            if dx == 0:
                send(w, q, at_col(1, 0))
                send(w, q, at_col(-1, 0))
                if dz == -1:
                    send(w, q, at_col(0, 1), first=0, count=32, recv=sem_half.at[0])
                if dz == 1:
                    send(w, q, at_col(0, -1), first=32, count=16, recv=sem_half.at[1])
            if dx == -1 and dz in (0, -1):
                send(w, q, at_col(1, 0))
            if dx == 1 and dz in (1, 2):
                send(w, q, at_col(-1, 0))
            send(w, q, to_row(w))
            send(w, q, partner)

    def rows():
        qy = ((y + 1) % 2) * 2 + core
        for d in ORDER:
            arrived(number(*d), qy)
            send(number(*d), qy, partner)

    def sides():
        for d in ORDER:
            arrived(number(*d), (y % 2) * 2 + 1 - core)
        for d in ORDER:
            arrived(number(*d), ((y + 1) % 2) * 2 + 1 - core)

    def finish():
        for c in sends:
            c.wait_send()

    return begin, plane, rows, sides, finish


def iota(shape, axis):
    return lax.broadcasted_iota(jnp.int32, shape, axis)


def one_hot(index, width):
    return jnp.where(iota((index.shape[0], width), 1) == index, 1.0, 0.0).astype(BF16)


def pick(selector, rows):
    return jnp.dot(selector, rows, preferred_element_type=F32)


def times_rows(left, right):
    return lax.dot_general(left, right, (((1,), (1,)), ((), ())), preferred_element_type=F32)


def cell_slot(i, j):
    return jnp.where(j < 16, 16 * i + j, 304 + 4 * i + j)


def window_slot(u, v):
    slot = ((u >> 3) * 2 + (v >> 3)) * 64 + (u & 7) * 8 + (v & 7)
    inside = (u >= 0) & (u < 16) & (v >= 0) & (v < 16)
    return jnp.where(inside, slot, -1)


def block_kernel(
    comb, mod_own, states, shifts, out_ref,
    weights, out_rows, mods, modv, ext, pack, normed, triples, att, back, result,
    sem_own, sem_send, sem_recv, sem_half, sem_ms, sem_mr,
    sem_x, sem_hs, sem_hr, sem_bs, sem_br, sem_ps, sem_pr, sem_o,
):
    row, col, y, core, x, z = place()
    section = lax.axis_index("section")
    begin, plane, rows, sides, finish = gather_weights(
        comb, weights, sem_own, sem_send, sem_recv, sem_half
    )
    row_up, row_down = (row + 1) % 16, (row + 15) % 16
    col_up, col_down = (col + 1) % 16, (col + 15) % 16

    barrier = pltpu.get_barrier_semaphore()
    peers = [{"wcol": (col + k) % 16} for k in range(1, 16)]
    near = [
        {"wrow": y * 2 + 1 - core},
        {"wrow": ((y + 1) % 8) * 2 + core},
        {"wrow": ((y + 7) % 8) * 2 + core},
        {"wrow": (row + 2 * core + 15) % 16},
        {"wrow": row_up, "wcol": col_up},
        {"wrow": row_down, "wcol": col_down},
        {"section": 1 - section},
    ]
    for peer in peers + near:
        pl.semaphore_signal(barrier, inc=1, device_id=peer, device_id_type=MESH)
    pl.semaphore_wait(barrier, len(peers) + len(near))

    def remote(source, target, send_sem, recv_sem, device):
        return pltpu.make_async_remote_copy(
            src_ref=source,
            dst_ref=target,
            send_sem=send_sem,
            recv_sem=recv_sem,
            device_id=device,
            device_id_type=MESH,
        )

    begin()

    def own_state(b):
        return pltpu.make_async_copy(states.at[b], ext.at[b, pl.ds(0, 256), :], sem_x.at[b])

    def state_copy(b):
        return remote(
            result.at[b], ext.at[b, pl.ds(0, 256), :], sem_ps.at[b], sem_pr.at[b],
            {"section": 1 - section},
        )

    def borders(b):
        def piece(k, source, first, count, device):
            return remote(
                source, ext.at[b, pl.ds(first, count), :], sem_hs.at[3 * b + k],
                sem_hr.at[3 * b + k], device,
            )

        return (
            piece(0, ext.at[b, pl.ds(0, 64), :], 256, 64, {"wrow": row_down}),
            piece(1, pack.at[b], 320, 64, {"wcol": col_down}),
            piece(2, pack.at[b, pl.ds(0, 16), :], 384, 16, {"wrow": row_down, "wcol": col_down}),
        )

    def returns(b):
        def piece(k, at, first, count, device):
            return remote(
                back.at[b, pl.ds(at, count), :], att.at[b, pl.ds(first, count), :],
                sem_bs.at[3 * b + k], sem_br.at[3 * b + k], device,
            )

        return (
            piece(0, 0, 256, 64, {"wrow": row_up}),
            piece(1, 64, 320, 64, {"wcol": col_up}),
            piece(2, 128, 384, 16, {"wrow": row_up, "wcol": col_up}),
        )

    def send_borders(b):
        t = iota((64, 1), 0)
        selector = one_hot((t >> 2) * 16 + (t & 3), 256)
        pack[b] = pick(selector, ext[b, 0:256, :]).astype(BF16)
        for c in borders(b):
            c.start()

    @pl.when(section == 0)
    def _():
        for b in range(MB):
            own_state(b).start()
        for b in range(MB):
            own_state(b).wait()
            send_borders(b)

    mods[pl.ds(col, 1)] = mod_own[...][None]
    msends = []
    for k in range(1, 16):
        c = remote(mod_own, mods.at[col], sem_ms.at[k], sem_mr.at[col], peers[k - 1])
        c.start()
        msends.append(c)

    for b in range(MB):
        ext[b, 400:512, :] = jnp.zeros((112, D), BF16)
        att[b, 400:512, :] = jnp.zeros((112, HEADS * HD), BF16)

    plane()
    rows()
    for k in range(1, 16):
        other = (col + k) % 16
        remote(mod_own, mods.at[other], sem_ms.at[k], sem_mr.at[other], peers[k - 1]).wait_recv()

    pieces = mods[...].reshape(16 * 24, 128).astype(BF16)
    lane = iota((40, 128), 1) >> 5
    for b in range(MB):
        joined = jnp.zeros((40, 128), F32)
        for k in range(4):
            piece = iota((40, 1), 0) * 4 + k
            shard = (piece * 57) >> 9
            index = jnp.where(piece < 144, 24 * shard + 9 * b + piece - 9 * shard, -1)
            joined = jnp.where(lane == k, pick(one_hot(index, 384), pieces), joined)
        for t in range(36):
            modv[b, :, 128 * t : 128 * t + 128] = jnp.broadcast_to(joined[t : t + 1], (8, 128))

    sides()
    for w in range(16):
        packed = weights[2304 + UNIT * w : 2304 + UNIT * w + UNIT, :]
        out_rows[96 * w : 96 * w + 48, :] = packed[:, :768]
        out_rows[96 * w + 48 : 96 * w + 96, :] = packed[:, 768:]

    r, c = shifts[0, 0], shifts[0, 1]

    def compute(b):
        for copy in borders(b):
            copy.wait_recv()
        scale = 1.0 + modv[b, 0:1, D : 2 * D]
        shift = modv[b, 0:1, 0:D]

        def normalize(window, carry):
            t = iota((64, 1), 0)
            i = r + 8 * (window >> 1) + (t >> 3)
            j = c + 8 * (window & 1) + (t & 7)
            values = pick(one_hot(cell_slot(i, j), 512), ext[b])
            center = values - jnp.mean(values, axis=-1, keepdims=True)
            spread = jnp.mean(center * center, axis=-1, keepdims=True)
            center = center * lax.rsqrt(spread + EPSILON)
            normed[pl.ds(pl.multiple_of(64 * window, 64), 64), :] = (center * scale + shift).astype(
                BF16
            )
            return carry

        lax.fori_loop(0, 4, normalize, 0)

        def project(k, carry):
            at = pl.multiple_of(256 * k, 256)
            triples[:, pl.ds(at, 256)] = times_rows(
                normed[...], weights[pl.ds(at, 256), :]
            ).astype(BF16)
            return carry

        lax.fori_loop(0, 9, project, 0)

        same = (iota((128, 128), 0) >> 6) == (iota((128, 128), 1) >> 6)
        for head in range(HEADS):
            for pair in range(2):
                here = slice(128 * pair, 128 * pair + 128)
                query, key, value = (
                    triples[here, 768 * n + HD * head : 768 * n + HD * head + HD] for n in range(3)
                )
                scores = times_rows(query, key) * HD ** (-0.5)
                powers = jnp.where(same, jnp.exp(jnp.where(same, scores, 0.0)), 0.0)
                total = jnp.sum(powers, axis=-1, keepdims=True)
                chances = (powers / total).astype(BF16)
                att[b, here, HD * head : HD * head + HD] = pick(chances, value).astype(BF16)

        t = iota((144, 1), 0)
        s = t - 64
        q = t - 128
        i = jnp.where(t < 64, 16 + (t >> 4), jnp.where(t < 128, s >> 2, 16 + (q >> 2)))
        j = jnp.where(t < 64, t & 15, 16 + (t & 3))
        back[b] = pick(one_hot(window_slot(i - r, j - c), 256), att[b, 0:256, :]).astype(BF16)
        for copy in returns(b):
            copy.start()

    def complete(b):
        for copy in returns(b):
            copy.wait_recv()
        t = iota((256, 1), 0)
        i, j = t >> 4, t & 15
        index = jnp.where(
            i >= r,
            jnp.where(j >= c, window_slot(i - r, j - c), 320 + 4 * i + j),
            jnp.where(j >= c, 256 + 16 * i + j, 384 + 4 * i + j),
        )
        normed[:, 0:768] = pick(one_hot(index, 512), att[b]).astype(BF16)

        def project(k, carry):
            at = pl.multiple_of(256 * k, 256)
            projection = times_rows(normed[:, 0:768], out_rows[pl.ds(at, 256), :]).astype(BF16)
            gate = modv[b, 0:1, pl.ds(pl.multiple_of(2 * D + 256 * k, 256), 256)]
            kept = ext[b, 0:256, pl.ds(at, 256)].astype(F32)
            result[b, :, pl.ds(at, 256)] = (kept + gate * projection.astype(F32)).astype(BF16)
            return carry

        lax.fori_loop(0, 6, project, 0)
        pltpu.make_async_copy(result.at[b], out_ref.at[b], sem_o.at[b]).start()

        @pl.when(section == 0)
        def _():
            state_copy(b).start()

    def receive(b):
        @pl.when(section == 1)
        def _():
            state_copy(b).wait_recv()
            send_borders(b)

    receive(0)
    compute(0)

    @pl.when(section == 0)
    def _():
        compute(1)

    receive(1)
    complete(0)

    @pl.when(section == 1)
    def _():
        compute(1)

    complete(1)

    for b in range(MB):
        for copy in borders(b) + returns(b):
            copy.wait_send()
        pltpu.make_async_copy(result.at[b], out_ref.at[b], sem_o.at[b]).wait()

    @pl.when(section == 0)
    def _():
        for b in range(MB):
            state_copy(b).wait_send()

    finish()
    for copy in msends:
        copy.wait_send()


def blocks(comb, mod_own, states, shifts):
    dma = pltpu.SemaphoreType.DMA
    return pl.pallas_call(
        block_kernel,
        out_shape=jax.ShapeDtypeStruct((MB, 256, D), BF16),
        in_specs=[
            pl.BlockSpec(memory_space=pl.ANY),
            pl.BlockSpec(memory_space=pltpu.VMEM),
            pl.BlockSpec(memory_space=pl.ANY),
            pl.BlockSpec(memory_space=pltpu.SMEM),
        ],
        out_specs=pl.BlockSpec(memory_space=pl.ANY),
        scratch_shapes=[
            pltpu.VMEM((3072, D), BF16),
            pltpu.VMEM((D, 768), BF16),
            pltpu.VMEM((16, 24, 128), F32),
            pltpu.VMEM((MB, 8, 3 * D), F32),
            pltpu.VMEM((MB, 512, D), BF16),
            pltpu.VMEM((MB, 64, D), BF16),
            pltpu.VMEM((256, D), BF16),
            pltpu.VMEM((256, 2304), BF16),
            pltpu.VMEM((MB, 512, 768), BF16),
            pltpu.VMEM((MB, 144, 768), BF16),
            pltpu.VMEM((MB, 256, D), BF16),
            dma((4,)),
            dma((68,)),
            dma((64,)),
            dma((2,)),
            dma((16,)),
            dma((16,)),
            dma((MB,)),
            dma((3 * MB,)),
            dma((3 * MB,)),
            dma((3 * MB,)),
            dma((3 * MB,)),
            dma((MB,)),
            dma((MB,)),
            dma((MB,)),
        ],
        compiler_params=pltpu.CompilerParams(
            collective_id=0, has_side_effects=True, vmem_limit_bytes=56 << 20
        ),
        name="blocks",
    )(comb, mod_own, states, shifts)


def packed_modulation(mod_part):
    pieces = mod_part.astype(jnp.float32).reshape(MB * 9, 32)
    return jnp.pad(jnp.tile(pieces, (1, 4)), ((0, 6), (0, 0)))


def per_device(states, timesteps, shifts, qkv_weight, out_weight, mod_weight):
    embedding = jax.nn.silu(sinusoid(timesteps, TEMB)).astype(jnp.bfloat16)
    mod_part = jnp.dot(embedding, mod_weight[0], preferred_element_type=jnp.float32).astype(
        jnp.bfloat16
    )
    out_rows = out_weight[0].T
    comb = jnp.concatenate(
        [qkv_weight[0].T, jnp.concatenate([out_rows[:UNIT], out_rows[UNIT:]], axis=1)], axis=0
    )
    results = blocks(comb, packed_modulation(mod_part), states.reshape(MB, 256, D), shifts)
    return results.reshape((1,) + states.shape)


def solution(mesh):
    in_specs = (
        P(None, "wrow", "wcol", None),
        P(),
        P("section", None),
        P("section", None, "wcol"),
        P("section", None, "wcol"),
        P("section", None, "wcol"),
    )
    out_specs = P("section", None, "wrow", "wcol", None)
    return jax.shard_map(
        per_device, mesh=mesh, in_specs=in_specs, out_specs=out_specs, check_vma=False
    )
```

```python
import math

import jax
import jax.numpy as jnp
from jax import lax
from jax.experimental import pallas as pl
from jax.experimental.pallas import tpu as pltpu
from jax.sharding import PartitionSpec as P

HEADS = 6
HD = 128
TEMB = 256
MB = 2
D = 1536
MESH = pl.DeviceIdType.MESH
UNIT = 48
EPSILON = 1e-06
BF16 = jnp.bfloat16
F32 = jnp.float32


def sinusoid(moments, entries):
    half_count = entries // 2
    frequency = jnp.exp(-math.log(10000.0) * jnp.arange(half_count, dtype=jnp.float32) / half_count)
    angles = moments.astype(jnp.float32)[:, None] * frequency[None, :]
    return jnp.concatenate([jnp.cos(angles), jnp.sin(angles)], axis=1)


def unit_row(w, q):
    last = q // 3
    return (144 * w + UNIT * q) * (1 - last) + (2304 + UNIT * w) * last


ORDER = (
    (0, -1), (0, 1), (-1, 0), (1, 0), (0, 2), (-1, -1), (1, -1), (-1, 1), (1, 1),
    (-1, 2), (1, 2), (2, 0), (2, -1), (2, 1), (2, 2),
)


def place():
    row, col = lax.axis_index("wrow"), lax.axis_index("wcol")
    return row, col, row // 2, row % 2, col // 4, col % 4


def gather_weights(comb, weights, sem_own, sem_send, sem_recv, sem_half):
    row, col, y, core, x, z = place()
    q = (y % 2) * 2 + core
    counter = [0]
    sends = []

    def unit(w, quarter, first=0, count=UNIT):
        start = pl.multiple_of(unit_row(w, quarter) + first, 16)
        return weights.at[pl.ds(start, count), :]

    def copy(w, quarter, target, slot, first=0, count=UNIT, recv=None):
        part = unit(w, quarter, first, count)
        return pltpu.make_async_remote_copy(
            src_ref=part,
            dst_ref=part,
            send_sem=sem_send.at[slot],
            recv_sem=sem_recv.at[w * 4 + quarter] if recv is None else recv,
            device_id=target,
            device_id_type=MESH,
        )

    def send(w, quarter, target, **kw):
        c = copy(w, quarter, target, counter[0], **kw)
        counter[0] += 1
        c.start()
        sends.append(c)

    def arrived(w, quarter, **kw):
        copy(w, quarter, {"wrow": row}, 0, **kw).wait_recv()

    def at_col(dx, dz):
        return {"wcol": ((x + dx + 4) % 4) * 4 + (z + dz + 4) % 4}

    partner = {"wrow": y * 2 + 1 - core}

    def number(dx, dz):
        return ((x + dx + 4) % 4) * 4 + (z + dz + 4) % 4

    def to_row(w):
        up = (w // 4 + w % 4) % 2
        return {"wrow": ((y + 7 + 2 * up) % 8) * 2 + core}

    own = []
    for quarter in range(4):
        c = pltpu.make_async_copy(
            comb.at[pl.ds(UNIT * quarter, UNIT), :], unit(col, quarter), sem_own.at[quarter]
        )
        c.start()
        own.append(c)

    def begin():
        for c in own:
            c.wait()
        for d in ((0, 1), (0, -1), (1, 0), (-1, 0)):
            send(col, q, at_col(*d))

    def plane():
        for dx, dz in ORDER:
            w = number(dx, dz)
            if (dx, dz) == (0, 2):
                arrived(w, q, first=0, count=32, recv=sem_half.at[0])
                arrived(w, q, first=32, count=16, recv=sem_half.at[1])
            else:
                arrived(w, q)
            if dx == 0:
                send(w, q, at_col(1, 0))
                send(w, q, at_col(-1, 0))
                if dz == -1:
                    send(w, q, at_col(0, 1), first=0, count=32, recv=sem_half.at[0])
                if dz == 1:
                    send(w, q, at_col(0, -1), first=32, count=16, recv=sem_half.at[1])
            if dx == -1 and dz in (0, -1):
                send(w, q, at_col(1, 0))
            if dx == 1 and dz in (1, 2):
                send(w, q, at_col(-1, 0))
            send(w, q, to_row(w))
            send(w, q, partner)

    def rows():
        qy = ((y + 1) % 2) * 2 + core
        for d in ORDER:
            arrived(number(*d), qy)
            send(number(*d), qy, partner)

    def sides():
        for d in ORDER:
            arrived(number(*d), (y % 2) * 2 + 1 - core)
        for d in ORDER:
            arrived(number(*d), ((y + 1) % 2) * 2 + 1 - core)

    def finish():
        for c in sends:
            c.wait_send()

    return begin, plane, rows, sides, finish


def iota(shape, axis):
    return lax.broadcasted_iota(jnp.int32, shape, axis)


def one_hot(index, width):
    return jnp.where(iota((index.shape[0], width), 1) == index, 1.0, 0.0).astype(BF16)


def pick(selector, rows):
    return jnp.dot(selector, rows, preferred_element_type=F32)


def times_rows(left, right):
    return lax.dot_general(left, right, (((1,), (1,)), ((), ())), preferred_element_type=F32)


def cell_slot(i, j):
    return jnp.where(j < 16, 16 * i + j, 304 + 4 * i + j)


def window_slot(u, v):
    slot = ((u >> 3) * 2 + (v >> 3)) * 64 + (u & 7) * 8 + (v & 7)
    inside = (u >= 0) & (u < 16) & (v >= 0) & (v < 16)
    return jnp.where(inside, slot, -1)


def block_kernel(
    comb, mod_own, states, shifts, out_ref,
    weights, out_rows, first_packed, first_rows, mods, modv, gates, first_gates,
    ext, pack, spread_in, spread_back, spread_own, spread_rim,
    rolled, normed, triples, att, rim, back, handed, result,
    sem_own, sem_send, sem_recv, sem_half, sem_ms, sem_mr,
    sem_x, sem_hs, sem_hr, sem_bs, sem_br, sem_ps, sem_pr, sem_o, sem_fs, sem_fr, sem_gs,
):
    row, col, y, core, x, z = place()
    section = lax.axis_index("section")
    begin, plane, rows, sides, finish = gather_weights(
        comb, weights, sem_own, sem_send, sem_recv, sem_half
    )
    row_up, row_down = (row + 1) % 16, (row + 15) % 16
    col_up, col_down = (col + 1) % 16, (col + 15) % 16
    col_before = x * 4 + (z + 3) % 4

    barrier = pltpu.get_barrier_semaphore()
    peers = [{"wcol": (col + k) % 16} for k in range(1, 16)]
    near = [
        {"wrow": y * 2 + 1 - core},
        {"wrow": ((y + 1) % 8) * 2 + core},
        {"wrow": ((y + 7) % 8) * 2 + core},
        {"wrow": (row + 2 * core + 15) % 16},
        {"wrow": row_up, "wcol": col_up},
        {"wrow": row_down, "wcol": col_down},
        {"section": 1 - section},
        {"section": 1 - section, "wcol": x * 4 + (z + 3 + 2 * section) % 4},
    ]
    for peer in peers + near:
        pl.semaphore_signal(barrier, inc=1, device_id=peer, device_id_type=MESH)
    pl.semaphore_wait(barrier, len(peers) + len(near))

    def remote(source, target, send_sem, recv_sem, device):
        return pltpu.make_async_remote_copy(
            src_ref=source,
            dst_ref=target,
            send_sem=send_sem,
            recv_sem=recv_sem,
            device_id=device,
            device_id_type=MESH,
        )

    begin()

    def own_state(b, target):
        return pltpu.make_async_copy(states.at[b], target, sem_x.at[b])

    def hand_over(b):
        return remote(
            handed.at[b], handed.at[b], sem_ps.at[b], sem_pr.at[b], {"section": 1 - section}
        )

    def hand_gates():
        return remote(gates, first_gates, sem_gs.at[0], sem_gs.at[1], {"section": 1 - section})

    def first_unit(slot, w, device):
        part = pl.ds(pl.multiple_of(UNIT * w, 16), UNIT)
        return remote(
            weights.at[pl.ds(pl.multiple_of(2304 + UNIT * w, 16), UNIT), :],
            first_packed.at[part, :], sem_fs.at[slot], sem_fr.at[w], device,
        )

    def relay_unit(slot, w):
        part = pl.ds(pl.multiple_of(UNIT * w, 16), UNIT)
        return remote(
            first_packed.at[part, :], first_packed.at[part, :], sem_fs.at[slot], sem_fr.at[w],
            {"wrow": y * 2 + 1 - core},
        )

    def first_sends():
        ahead = [first_unit(k, 2 * k + core, {"section": 1 - section}) for k in range(4)]
        behind = [
            first_unit(k, 2 * k + core, {"section": 1 - section, "wcol": col_before})
            for k in range(4, 8)
        ]
        return ahead + behind

    def borders(b):
        def piece(k, source, first, count, device):
            return remote(
                source, ext.at[b, pl.ds(first, count), :], sem_hs.at[3 * b + k],
                sem_hr.at[3 * b + k], device,
            )

        return (
            piece(0, ext.at[b, pl.ds(0, 64), :], 256, 64, {"wrow": row_down}),
            piece(1, pack.at[b], 320, 64, {"wcol": col_down}),
            piece(2, pack.at[b, pl.ds(0, 16), :], 384, 16, {"wrow": row_down, "wcol": col_down}),
        )

    def returns(b):
        def piece(k, at, count, device):
            part = pl.ds(at, count)
            return remote(
                back.at[b, part, :], rim.at[b, part, :],
                sem_bs.at[3 * b + k], sem_br.at[3 * b + k], device,
            )

        return (
            piece(0, 0, 64, {"wrow": row_up}),
            piece(1, 64, 64, {"wcol": col_up}),
            piece(2, 128, 16, {"wrow": row_up, "wcol": col_up}),
        )

    def send_borders(b):
        t = iota((64, 1), 0)
        selector = one_hot((t >> 2) * 16 + (t & 3), 256)
        pack[b] = pick(selector, ext[b, 0:256, :]).astype(BF16)
        for c in borders(b):
            c.start()

    @pl.when(section == 0)
    def _():
        for b in range(MB):
            own_state(b, ext.at[b, pl.ds(0, 256), :]).start()
        for b in range(MB):
            own_state(b, ext.at[b, pl.ds(0, 256), :]).wait()
            send_borders(b)

    @pl.when(section == 1)
    def _():
        for b in range(MB):
            own_state(b, result.at[b]).start()

    mods[pl.ds(col, 1)] = mod_own[...][None]
    msends = []
    for k in range(1, 16):
        c = remote(mod_own, mods.at[col], sem_ms.at[k], sem_mr.at[col], peers[k - 1])
        c.start()
        msends.append(c)

    for b in range(MB):
        ext[b, 400:512, :] = jnp.zeros((112, D), BF16)
        rim[b, 144:256, :] = jnp.zeros((112, HEADS * HD), BF16)

    r, c = shifts[0, 0], shifts[0, 1]
    t = iota((256, 1), 0)
    i = r + 8 * (t >> 7) + ((t >> 3) & 7)
    j = c + 8 * ((t >> 6) & 1) + (t & 7)
    spread_in[...] = one_hot(cell_slot(i, j), 512)
    i, j = t >> 4, t & 15
    spread_own[...] = one_hot(window_slot(i - r, j - c), 256)
    index = jnp.where(
        i >= r,
        jnp.where(j >= c, -1, 64 + 4 * i + j),
        jnp.where(j >= c, 16 * i + j, 128 + 4 * i + j),
    )
    spread_rim[...] = one_hot(index, 256)
    t = iota((144, 1), 0)
    s = t - 64
    q = t - 128
    i = jnp.where(t < 64, 16 + (t >> 4), jnp.where(t < 128, s >> 2, 16 + (q >> 2)))
    j = jnp.where(t < 64, t & 15, 16 + (t & 3))
    spread_back[...] = one_hot(window_slot(i - r, j - c), 256)

    plane()
    rows()
    for k in range(1, 16):
        other = (col + k) % 16
        remote(mod_own, mods.at[other], sem_ms.at[k], sem_mr.at[other], peers[k - 1]).wait_recv()

    pieces = mods[...].reshape(16 * 24, 128).astype(BF16)
    lane = iota((40, 128), 1) >> 5
    gates[...] = jnp.zeros((8, D), F32)
    for b in range(MB):
        joined = jnp.zeros((40, 128), F32)
        for k in range(4):
            piece = iota((40, 1), 0) * 4 + k
            shard = (piece * 57) >> 9
            index = jnp.where(piece < 144, 24 * shard + 9 * b + piece - 9 * shard, -1)
            joined = jnp.where(lane == k, pick(one_hot(index, 384), pieces), joined)
        for t in range(24):
            modv[b, :, 128 * t : 128 * t + 128] = jnp.broadcast_to(joined[t : t + 1], (8, 128))
        for t in range(12):
            gates[b : b + 1, 128 * t : 128 * t + 128] = joined[24 + t : 25 + t]

    sides()

    @pl.when(section == 0)
    def _():
        hand_gates().start()
        for copy in first_sends():
            copy.start()

    def unpack(source, base, target):
        for w in range(16):
            packed = source[base + UNIT * w : base + UNIT * w + UNIT, :]
            target[96 * w : 96 * w + 48, :] = packed[:, :768]
            target[96 * w + 48 : 96 * w + 96, :] = packed[:, 768:]

    def add_projection(source, matrix, gate, kept, target):
        for k in range(6):
            here = slice(256 * k, 256 * k + 256)
            projection = times_rows(source, matrix[here, :]).astype(BF16)
            target[:, here] = (
                kept[:, here].astype(F32) + gate[:, here] * projection.astype(F32)
            ).astype(BF16)

    def compute(b):
        for copy in borders(b):
            copy.wait_recv()
        for k in range(3):
            here = slice(512 * k, 512 * k + 512)
            rolled[:, here] = pick(spread_in[...], ext[b, :, here]).astype(BF16)
        scale = 1.0 + modv[b, 0:1, D : 2 * D]
        shift = modv[b, 0:1, 0:D]
        for k in range(8):
            here = slice(32 * k, 32 * k + 32)
            values = rolled[here, :].astype(F32)
            center = values - jnp.mean(values, axis=-1, keepdims=True)
            spread = jnp.mean(center * center, axis=-1, keepdims=True)
            center = center * lax.rsqrt(spread + EPSILON)
            normed[here, :] = (center * scale + shift).astype(BF16)
        for k in range(3):
            here = slice(768 * k, 768 * k + 768)
            triples[here, :] = times_rows(weights[here, :], normed[...]).astype(BF16)

        same = (iota((128, 128), 0) >> 6) == (iota((128, 128), 1) >> 6)
        for head in range(HEADS):
            for pair in range(2):
                here = slice(128 * pair, 128 * pair + 128)
                query, key, value = (
                    triples[768 * n + HD * head : 768 * n + HD * head + HD, here] for n in range(3)
                )
                scores = lax.dot_general(
                    key, query, (((0,), (0,)), ((), ())), preferred_element_type=F32
                ) * HD ** (-0.5)
                powers = jnp.where(same, jnp.exp(jnp.where(same, scores, 0.0)), 0.0)
                total = jnp.sum(powers, axis=0, keepdims=True)
                chances = (powers / total).astype(BF16)
                att[b, HD * head : HD * head + HD, here] = pick(value, chances).astype(BF16)

        back[b] = times_rows(spread_back[...], att[b]).astype(BF16)
        for copy in returns(b):
            copy.start()

    def complete(b):
        for copy in returns(b):
            copy.wait_recv()
        own = times_rows(spread_own[...], att[b])
        handed[b] = (own + pick(spread_rim[...], rim[b])).astype(BF16)

        @pl.when(section == 0)
        def _():
            hand_over(b).start()

        add_projection(
            handed[b], out_rows, gates[b : b + 1, :], ext.at[b, pl.ds(0, 256), :], result.at[b]
        )
        pltpu.make_async_copy(result.at[b], out_ref.at[b], sem_o.at[b]).start()

    unpack(weights, 2304, out_rows)

    @pl.when(section == 1)
    def _():
        for k in range(8):
            first_unit(k, 2 * k + core, {"section": 1 - section}).wait_recv()
            relay_unit(k, 2 * k + core).start()
        for k in range(8):
            relay_unit(k, 2 * k + 1 - core).wait_recv()
        unpack(first_packed, 0, first_rows)
        hand_gates().wait_recv()
        for b in range(MB):
            own_state(b, result.at[b]).wait()
            hand_over(b).wait_recv()
            add_projection(
                handed[b], first_rows, first_gates[b : b + 1, :], result.at[b],
                ext.at[b, pl.ds(0, 256), :],
            )
            send_borders(b)

    for b in range(MB):
        compute(b)
    for b in range(MB):
        complete(b)

    for b in range(MB):
        for copy in borders(b) + returns(b):
            copy.wait_send()
        pltpu.make_async_copy(result.at[b], out_ref.at[b], sem_o.at[b]).wait()

    @pl.when(section == 0)
    def _():
        for b in range(MB):
            hand_over(b).wait_send()
        hand_gates().wait_send()
        for copy in first_sends():
            copy.wait_send()

    @pl.when(section == 1)
    def _():
        for k in range(8):
            relay_unit(k, 2 * k + core).wait_send()

    finish()
    for copy in msends:
        copy.wait_send()


def blocks(comb, mod_own, states, shifts):
    dma = pltpu.SemaphoreType.DMA
    return pl.pallas_call(
        block_kernel,
        out_shape=jax.ShapeDtypeStruct((MB, 256, D), BF16),
        in_specs=[
            pl.BlockSpec(memory_space=pl.ANY),
            pl.BlockSpec(memory_space=pltpu.VMEM),
            pl.BlockSpec(memory_space=pl.ANY),
            pl.BlockSpec(memory_space=pltpu.SMEM),
        ],
        out_specs=pl.BlockSpec(memory_space=pl.ANY),
        scratch_shapes=[
            pltpu.VMEM((3072, D), BF16),
            pltpu.VMEM((D, 768), BF16),
            pltpu.VMEM((768, D), BF16),
            pltpu.VMEM((D, 768), BF16),
            pltpu.VMEM((16, 24, 128), F32),
            pltpu.VMEM((MB, 8, 2 * D), F32),
            pltpu.VMEM((8, D), F32),
            pltpu.VMEM((8, D), F32),
            pltpu.VMEM((MB, 512, D), BF16),
            pltpu.VMEM((MB, 64, D), BF16),
            pltpu.VMEM((256, 512), BF16),
            pltpu.VMEM((144, 256), BF16),
            pltpu.VMEM((256, 256), BF16),
            pltpu.VMEM((256, 256), BF16),
            pltpu.VMEM((256, D), BF16),
            pltpu.VMEM((256, D), BF16),
            pltpu.VMEM((2304, 256), BF16),
            pltpu.VMEM((MB, 768, 256), BF16),
            pltpu.VMEM((MB, 256, 768), BF16),
            pltpu.VMEM((MB, 144, 768), BF16),
            pltpu.VMEM((MB, 256, 768), BF16),
            pltpu.VMEM((MB, 256, D), BF16),
            dma((4,)),
            dma((68,)),
            dma((64,)),
            dma((2,)),
            dma((16,)),
            dma((16,)),
            dma((MB,)),
            dma((3 * MB,)),
            dma((3 * MB,)),
            dma((3 * MB,)),
            dma((3 * MB,)),
            dma((MB,)),
            dma((MB,)),
            dma((MB,)),
            dma((8,)),
            dma((16,)),
            dma((2,)),
        ],
        compiler_params=pltpu.CompilerParams(
            collective_id=0, has_side_effects=True, vmem_limit_bytes=60 << 20
        ),
        name="blocks",
    )(comb, mod_own, states, shifts)


def packed_modulation(mod_part):
    pieces = mod_part.astype(jnp.float32).reshape(MB * 9, 32)
    return jnp.pad(jnp.tile(pieces, (1, 4)), ((0, 6), (0, 0)))


def per_device(states, timesteps, shifts, qkv_weight, out_weight, mod_weight):
    embedding = jax.nn.silu(sinusoid(timesteps, TEMB)).astype(jnp.bfloat16)
    mod_part = jnp.dot(embedding, mod_weight[0], preferred_element_type=jnp.float32).astype(
        jnp.bfloat16
    )
    out_rows = out_weight[0].T
    comb = jnp.concatenate(
        [qkv_weight[0].T, jnp.concatenate([out_rows[:UNIT], out_rows[UNIT:]], axis=1)], axis=0
    )
    results = blocks(comb, packed_modulation(mod_part), states.reshape(MB, 256, D), shifts)
    return results.reshape((1,) + states.shape)


def solution(mesh):
    in_specs = (
        P(None, "wrow", "wcol", None),
        P(),
        P("section", None),
        P("section", None, "wcol"),
        P("section", None, "wcol"),
        P("section", None, "wcol"),
    )
    out_specs = P("section", None, "wrow", "wcol", None)
    return jax.shard_map(
        per_device, mesh=mesh, in_specs=in_specs, out_specs=out_specs, check_vma=False
    )
```

```python
import math

import jax
import jax.numpy as jnp
from jax import lax
from jax.experimental import pallas as pl
from jax.experimental.pallas import tpu as pltpu
from jax.sharding import PartitionSpec as P

HEADS = 6
HD = 128
TEMB = 256
MB = 2
D = 1536
MESH = pl.DeviceIdType.MESH
UNIT = 48
EPSILON = 1e-06
BF16 = jnp.bfloat16
F32 = jnp.float32


def sinusoid(moments, entries):
    half_count = entries // 2
    frequency = jnp.exp(-math.log(10000.0) * jnp.arange(half_count, dtype=jnp.float32) / half_count)
    angles = moments.astype(jnp.float32)[:, None] * frequency[None, :]
    return jnp.concatenate([jnp.cos(angles), jnp.sin(angles)], axis=1)


def unit_row(w, q):
    last = q // 3
    return (144 * w + UNIT * q) * (1 - last) + (2304 + UNIT * w) * last


ORDER = (
    (0, -1), (0, 1), (-1, 0), (1, 0), (0, 2), (-1, -1), (1, -1), (-1, 1), (1, 1),
    (-1, 2), (1, 2), (2, 0), (2, -1), (2, 1), (2, 2),
)


def place():
    row, col = lax.axis_index("wrow"), lax.axis_index("wcol")
    return row, col, row // 2, row % 2, col // 4, col % 4


def gather_weights(qkv_t, out_t, weights, sem_own, sem_send, sem_piece, sem_unit):
    row, col, y, core, x, z = place()
    q = (y % 2) * 2 + core
    qy = ((y + 1) % 2) * 2 + core
    sends = []

    def number(dx, dz):
        return ((x + dx + 4) % 4) * 4 + (z + dz + 4) % 4

    def at_col(dx, dz):
        return {"wcol": number(dx, dz)}

    def to_row(w):
        up = (w // 4 + w % 4) % 2
        return {"wrow": ((y + 7 + 2 * up) % 8) * 2 + core}

    partner = {"wrow": y * 2 + 1 - core}

    def copy(w, quarter, target, slot, piece=None):
        first = 0 if piece is None else 16 * piece
        count = UNIT if piece is None else 16
        part = weights.at[pl.ds(pl.multiple_of(unit_row(w, quarter) + first, 16), count), :]
        return pltpu.make_async_remote_copy(
            src_ref=part,
            dst_ref=part,
            send_sem=sem_send.at[slot],
            recv_sem=sem_unit.at[w * 4 + quarter] if piece is None else sem_piece.at[w * 3 + piece],
            device_id=target,
            device_id_type=MESH,
        )

    def send(w, quarter, target, piece=None):
        c = copy(w, quarter, target, len(sends), piece)
        c.start()
        sends.append(c)

    def arrived(w, quarter, piece=None):
        copy(w, quarter, partner, 0, piece).wait_recv()

    def unit(w, quarter):
        return weights.at[pl.ds(pl.multiple_of(unit_row(w, quarter), 16), UNIT), :]

    own = [
        pltpu.make_async_copy(qkv_t.at[pl.ds(UNIT * k, UNIT), :], unit(col, k), sem_own.at[k])
        for k in range(3)
    ] + [
        pltpu.make_async_copy(
            out_t.at[pl.ds(UNIT * k, UNIT), :], unit(col, 3).at[:, pl.ds(768 * k, 768)],
            sem_own.at[3 + k],
        )
        for k in range(2)
    ]

    def load():
        for c in own:
            c.start()
        for c in own:
            c.wait()

    def begin():
        for piece in range(3):
            for d in ((0, 1), (0, -1), (1, 0), (-1, 0)):
                send(col, q, at_col(*d), piece)
        for d in ((1, 0), (-1, 0)):
            send(col, qy, at_col(*d))

    def plane(after_z):
        def event(dx, dz, piece):
            w = number(dx, dz)
            arrived(w, q, piece)
            if dz == -1 and dx == 0 and piece < 2:
                send(w, q, at_col(0, 1), piece)
            if dz == 1 and dx == 0 and piece == 2:
                send(w, q, at_col(0, -1), piece)
            if dx == 0:
                send(w, q, at_col(1, 0), piece)
                send(w, q, at_col(-1, 0), piece)
            if dx == -1 and dz in (0, -1):
                send(w, q, at_col(1, 0), piece)
            if dx == 1 and dz in (1, 2):
                send(w, q, at_col(-1, 0), piece)

        def whole(dx, dz):
            w = number(dx, dz)
            if dx == 0 or dz != 0 or dx == 2:
                send(w, q, to_row(w))
            send(w, q, partner)

        for group in (((0, -1), (0, 1), (-1, 0), (1, 0)), ((0, 2),)):
            for piece in range(3):
                for d in group:
                    event(*d, piece)
            for d in group:
                whole(*d)
        after_z()
        for d in ORDER[5:]:
            for piece in range(3):
                event(*d, piece)
            whole(*d)

    def rows():
        for d in ((-1, 0), (1, 0), (0, -1), (0, 1)) + ORDER[4:]:
            arrived(number(*d), qy)
            send(number(*d), qy, partner)

    def sides():
        for d in ORDER:
            arrived(number(*d), (y % 2) * 2 + 1 - core)
        for d in ORDER:
            arrived(number(*d), ((y + 1) % 2) * 2 + 1 - core)

    def finish():
        for c in sends:
            c.wait_send()

    return load, begin, plane, rows, sides, finish


def iota(shape, axis):
    return lax.broadcasted_iota(jnp.int32, shape, axis)


def one_hot(index, width):
    return jnp.where(iota((index.shape[0], width), 1) == index, 1.0, 0.0).astype(BF16)


def pick(selector, rows):
    return jnp.dot(selector, rows, preferred_element_type=F32)


def times_rows(left, right):
    return lax.dot_general(left, right, (((1,), (1,)), ((), ())), preferred_element_type=F32)


def cell_slot(i, j):
    return jnp.where(j < 16, 16 * i + j, 304 + 4 * i + j)


def window_slot(u, v):
    slot = ((u >> 3) * 2 + (v >> 3)) * 64 + (u & 7) * 8 + (v & 7)
    inside = (u >= 0) & (u < 16) & (v >= 0) & (v < 16)
    return jnp.where(inside, slot, -1)


def block_kernel(
    qkv_t, out_t, mod_own, states, shifts, out_ref,
    weights, out_rows, first_packed, first_rows, mods, modv, gates, first_gates,
    ext, pack, spread_in, spread_back, spread_own, spread_rim,
    rolled, normed, triples, att, rim, back, handed, result,
    sem_own, sem_send, sem_piece, sem_unit, sem_ms, sem_mr,
    sem_x, sem_hs, sem_hr, sem_bs, sem_br, sem_ps, sem_pr, sem_o, sem_fs, sem_fr, sem_gs,
    sem_cs, sem_go,
):
    row, col, y, core, x, z = place()
    section = lax.axis_index("section")
    load, begin, plane, rows, sides, finish = gather_weights(
        qkv_t, out_t, weights, sem_own, sem_send, sem_piece, sem_unit
    )
    row_up, row_down = (row + 1) % 16, (row + 15) % 16
    col_up, col_down = (col + 1) % 16, (col + 15) % 16

    barrier = pltpu.get_barrier_semaphore()
    peers = [{"wcol": (col + k) % 16} for k in range(1, 16)]
    near = [
        {"wrow": y * 2 + 1 - core},
        {"wrow": ((y + 1) % 8) * 2 + core},
        {"wrow": ((y + 7) % 8) * 2 + core},
        {"wrow": (row + 2 * core + 15) % 16},
        {"wrow": row_up, "wcol": col_up},
        {"wrow": row_down, "wcol": col_down},
        {"section": 1 - section},
        {"section": 1 - section, "wcol": (col + 15 + 2 * section) % 16},
        {
            "section": 1 - section,
            "wrow": (row + 15 + 2 * section) % 16,
            "wcol": (col + 15 + 2 * section) % 16,
        },
    ]
    for peer in peers + near:
        pl.semaphore_signal(barrier, inc=1, device_id=peer, device_id_type=MESH)
    load()
    pl.semaphore_wait(barrier, len(peers) + len(near))

    def remote(source, target, send_sem, recv_sem, device):
        return pltpu.make_async_remote_copy(
            src_ref=source,
            dst_ref=target,
            send_sem=send_sem,
            recv_sem=recv_sem,
            device_id=device,
            device_id_type=MESH,
        )

    def own_state(b, target):
        return pltpu.make_async_copy(states.at[b], target, sem_x.at[b])

    def hand_over(b):
        return remote(
            handed.at[b], handed.at[b], sem_ps.at[b], sem_pr.at[b], {"section": 1 - section}
        )

    def hand_gates():
        return remote(gates, first_gates, sem_gs.at[0], sem_gs.at[1], {"section": 1 - section})

    def first_unit(slot, w, device):
        part = pl.ds(pl.multiple_of(UNIT * w, 16), UNIT)
        return remote(
            weights.at[pl.ds(pl.multiple_of(2304 + UNIT * w, 16), UNIT), :],
            first_packed.at[part, :], sem_fs.at[slot], sem_fr.at[w], device,
        )

    def relay_unit(slot, w):
        part = pl.ds(pl.multiple_of(UNIT * w, 16), UNIT)
        return remote(
            first_packed.at[part, :], first_packed.at[part, :], sem_fs.at[slot], sem_fr.at[w],
            {"wrow": y * 2 + 1 - core},
        )

    def first_sends():
        ahead = [first_unit(k, 2 * k + core, {"section": 1 - section}) for k in range(4)]
        behind = [
            first_unit(k, 2 * k + core, {"section": 1 - section, "wcol": col_down})
            for k in range(4, 8)
        ]
        return ahead + behind

    def borders(b):
        def piece(k, source, first, count, device):
            return remote(
                source, ext.at[b, pl.ds(first, count), :], sem_hs.at[3 * b + k],
                sem_hr.at[3 * b + k], device,
            )

        return (
            piece(0, ext.at[b, pl.ds(0, 64), :], 256, 64, {"wrow": row_down}),
            piece(1, pack.at[b], 320, 64, {"wcol": col_down}),
            piece(2, pack.at[b, pl.ds(0, 16), :], 384, 16, {"wrow": row_down, "wcol": col_down}),
        )

    def returns(b):
        def piece(k, at, count, device):
            part = pl.ds(at, count)
            return remote(
                back.at[b, part, :], rim.at[b, part, :],
                sem_bs.at[3 * b + k], sem_br.at[3 * b + k], device,
            )

        return (
            piece(0, 0, 64, {"wrow": row_up}),
            piece(1, 64, 64, {"wcol": col_up}),
            piece(2, 128, 16, {"wrow": row_up, "wcol": col_up}),
        )

    def cross_borders(b):
        def piece(k, count, device):
            return remote(
                pack.at[b, pl.ds(0, count), :], ext.at[b, pl.ds(256 + 64 * k, count), :],
                sem_cs.at[2 * b + k - 1], sem_hr.at[3 * b + k], device,
            )

        return (
            piece(1, 64, {"section": 1 - section, "wcol": col_down}),
            piece(2, 16, {"section": 1 - section, "wrow": row_down, "wcol": col_down}),
        )

    def pack_columns(b, source):
        t = iota((64, 1), 0)
        selector = one_hot((t >> 2) * 16 + (t & 3), 256)
        pack[b] = pick(selector, source).astype(BF16)

    @pl.when(section == 0)
    def _():
        for b in range(MB):
            own_state(b, ext.at[b, pl.ds(0, 256), :]).start()

    @pl.when(section == 1)
    def _():
        for b in range(MB):
            own_state(b, result.at[b]).start()

    def go():
        pl.semaphore_signal(
            sem_go, inc=1, device_id={"section": 1 - section}, device_id_type=MESH
        )

    @pl.when(section == 1)
    def _():
        pl.semaphore_wait(sem_go, 1)

    begin()

    mods[pl.ds(col, 1)] = mod_own[...][None]
    msends = []
    for k in range(1, 16):
        c = remote(mod_own, mods.at[col], sem_ms.at[k], sem_mr.at[col], peers[k - 1])
        c.start()
        msends.append(c)

    for b in range(MB):
        ext[b, 400:512, :] = jnp.zeros((112, D), BF16)
        rim[b, 144:256, :] = jnp.zeros((112, HEADS * HD), BF16)

    r, c = shifts[0, 0], shifts[0, 1]
    t = iota((256, 1), 0)
    i = r + 8 * (t >> 7) + ((t >> 3) & 7)
    j = c + 8 * ((t >> 6) & 1) + (t & 7)
    spread_in[...] = one_hot(cell_slot(i, j), 512)
    i, j = t >> 4, t & 15
    spread_own[...] = one_hot(window_slot(i - r, j - c), 256)
    index = jnp.where(
        i >= r,
        jnp.where(j >= c, -1, 64 + 4 * i + j),
        jnp.where(j >= c, 16 * i + j, 128 + 4 * i + j),
    )
    spread_rim[...] = one_hot(index, 256)
    t = iota((144, 1), 0)
    s = t - 64
    q = t - 128
    i = jnp.where(t < 64, 16 + (t >> 4), jnp.where(t < 128, s >> 2, 16 + (q >> 2)))
    j = jnp.where(t < 64, t & 15, 16 + (t & 3))
    spread_back[...] = one_hot(window_slot(i - r, j - c), 256)

    def after_z():
        @pl.when(section == 0)
        def _():
            go()
            for b in range(MB):
                own_state(b, ext.at[b, pl.ds(0, 256), :]).wait()
                pack_columns(b, ext[b, 0:256, :])
                for copy in borders(b):
                    copy.start()

    plane(after_z)
    rows()
    for k in range(1, 16):
        other = (col + k) % 16
        remote(mod_own, mods.at[other], sem_ms.at[k], sem_mr.at[other], peers[k - 1]).wait_recv()

    pieces = mods[...].reshape(16 * 24, 128).astype(BF16)
    lane = iota((40, 128), 1) >> 5
    gates[...] = jnp.zeros((8, D), F32)
    for b in range(MB):
        joined = jnp.zeros((40, 128), F32)
        for k in range(4):
            piece = iota((40, 1), 0) * 4 + k
            shard = (piece * 57) >> 9
            index = jnp.where(piece < 144, 24 * shard + 9 * b + piece - 9 * shard, -1)
            joined = jnp.where(lane == k, pick(one_hot(index, 384), pieces), joined)
        for t in range(24):
            modv[b, :, 128 * t : 128 * t + 128] = jnp.broadcast_to(joined[t : t + 1], (8, 128))
        for t in range(12):
            gates[b : b + 1, 128 * t : 128 * t + 128] = joined[24 + t : 25 + t]

    def unpack(source, base, target):
        for w in range(16):
            packed = source[base + UNIT * w : base + UNIT * w + UNIT, :]
            target[96 * w : 96 * w + 48, :] = packed[:, :768]
            target[96 * w + 48 : 96 * w + 96, :] = packed[:, 768:]

    def add_projection(source, matrix, gate, kept, target):
        for k in range(6):
            here = slice(256 * k, 256 * k + 256)
            projection = times_rows(source, matrix[here, :]).astype(BF16)
            target[:, here] = (
                kept[:, here].astype(F32) + gate[:, here] * projection.astype(F32)
            ).astype(BF16)

    def prepare(b):
        for copy in borders(b):
            copy.wait_recv()
        for k in range(3):
            here = slice(512 * k, 512 * k + 512)
            rolled[:, here] = pick(spread_in[...], ext[b, :, here]).astype(BF16)
        scale = 1.0 + modv[b, 0:1, D : 2 * D]
        shift = modv[b, 0:1, 0:D]
        for k in range(8):
            here = slice(32 * k, 32 * k + 32)
            values = rolled[here, :].astype(F32)
            center = values - jnp.mean(values, axis=-1, keepdims=True)
            spread = jnp.mean(center * center, axis=-1, keepdims=True)
            center = center * lax.rsqrt(spread + EPSILON)
            normed[b, here, :] = (center * scale + shift).astype(BF16)
    def compute(b):
        for k in range(3):
            here = slice(768 * k, 768 * k + 768)
            triples[here, :] = times_rows(weights[here, :], normed[b]).astype(BF16)

        same = (iota((128, 128), 0) >> 6) == (iota((128, 128), 1) >> 6)
        for head in range(HEADS):
            for pair in range(2):
                here = slice(128 * pair, 128 * pair + 128)
                query, key, value = (
                    triples[768 * n + HD * head : 768 * n + HD * head + HD, here] for n in range(3)
                )
                scores = lax.dot_general(
                    key, query, (((0,), (0,)), ((), ())), preferred_element_type=F32
                ) * HD ** (-0.5)
                powers = jnp.where(same, jnp.exp(jnp.where(same, scores, 0.0)), 0.0)
                total = jnp.sum(powers, axis=0, keepdims=True)
                chances = (powers / total).astype(BF16)
                att[b, HD * head : HD * head + HD, here] = pick(value, chances).astype(BF16)

        back[b] = times_rows(spread_back[...], att[b]).astype(BF16)
        for copy in returns(b):
            copy.start()

    def complete(b):
        for copy in returns(b):
            copy.wait_recv()
        own = times_rows(spread_own[...], att[b])
        handed[b] = (own + pick(spread_rim[...], rim[b])).astype(BF16)

        @pl.when(section == 0)
        def _():
            hand_over(b).start()

        add_projection(
            handed[b], out_rows, gates[b : b + 1, :], ext.at[b, pl.ds(0, 256), :], result.at[b]
        )

        @pl.when(section == 0)
        def _():
            for copy in borders(b)[1:]:
                copy.wait_send()
            pack_columns(b, result[b])
            for copy in cross_borders(b):
                copy.start()

        pltpu.make_async_copy(result.at[b], out_ref.at[b], sem_o.at[b]).start()

    @pl.when(section == 0)
    def _():
        for b in range(MB):
            prepare(b)

    sides()

    @pl.when(section == 0)
    def _():
        hand_gates().start()
        for copy in first_sends():
            copy.start()

    @pl.when(section == 1)
    def _():
        for k in range(8):
            first_unit(k, 2 * k + core, {"section": 1 - section}).wait_recv()
            relay_unit(k, 2 * k + core).start()
        for k in range(8):
            relay_unit(k, 2 * k + 1 - core).wait_recv()
        unpack(first_packed, 0, first_rows)
        hand_gates().wait_recv()
        for b in range(MB):
            own_state(b, result.at[b]).wait()
            hand_over(b).wait_recv()
            add_projection(
                handed[b], first_rows, first_gates[b : b + 1, :], result.at[b],
                ext.at[b, pl.ds(0, 256), :],
            )
            borders(b)[0].start()
        for b in range(MB):
            prepare(b)

    for b in range(MB):
        compute(b)
    unpack(weights, 2304, out_rows)
    for b in range(MB):
        complete(b)

    for b in range(MB):
        borders(b)[0].wait_send()
        for copy in returns(b):
            copy.wait_send()
        pltpu.make_async_copy(result.at[b], out_ref.at[b], sem_o.at[b]).wait()

    @pl.when(section == 0)
    def _():
        for b in range(MB):
            hand_over(b).wait_send()
            for copy in cross_borders(b):
                copy.wait_send()
        hand_gates().wait_send()
        for copy in first_sends():
            copy.wait_send()

    @pl.when(section == 1)
    def _():
        for k in range(8):
            relay_unit(k, 2 * k + core).wait_send()

    finish()
    for copy in msends:
        copy.wait_send()


def blocks(qkv_t, out_t, mod_own, states, shifts):
    dma = pltpu.SemaphoreType.DMA
    return pl.pallas_call(
        block_kernel,
        out_shape=jax.ShapeDtypeStruct((MB, 256, D), BF16),
        in_specs=[
            pl.BlockSpec(memory_space=pl.ANY),
            pl.BlockSpec(memory_space=pl.ANY),
            pl.BlockSpec(memory_space=pltpu.VMEM),
            pl.BlockSpec(memory_space=pl.ANY),
            pl.BlockSpec(memory_space=pltpu.SMEM),
        ],
        out_specs=pl.BlockSpec(memory_space=pl.ANY),
        scratch_shapes=[
            pltpu.VMEM((3072, D), BF16),
            pltpu.VMEM((D, 768), BF16),
            pltpu.VMEM((768, D), BF16),
            pltpu.VMEM((D, 768), BF16),
            pltpu.VMEM((16, 24, 128), F32),
            pltpu.VMEM((MB, 8, 2 * D), F32),
            pltpu.VMEM((8, D), F32),
            pltpu.VMEM((8, D), F32),
            pltpu.VMEM((MB, 512, D), BF16),
            pltpu.VMEM((MB, 64, D), BF16),
            pltpu.VMEM((256, 512), BF16),
            pltpu.VMEM((144, 256), BF16),
            pltpu.VMEM((256, 256), BF16),
            pltpu.VMEM((256, 256), BF16),
            pltpu.VMEM((256, D), BF16),
            pltpu.VMEM((MB, 256, D), BF16),
            pltpu.VMEM((2304, 256), BF16),
            pltpu.VMEM((MB, 768, 256), BF16),
            pltpu.VMEM((MB, 256, 768), BF16),
            pltpu.VMEM((MB, 144, 768), BF16),
            pltpu.VMEM((MB, 256, 768), BF16),
            pltpu.VMEM((MB, 256, D), BF16),
            dma((5,)),
            dma((96,)),
            dma((48,)),
            dma((64,)),
            dma((16,)),
            dma((16,)),
            dma((MB,)),
            dma((3 * MB,)),
            dma((3 * MB,)),
            dma((3 * MB,)),
            dma((3 * MB,)),
            dma((MB,)),
            dma((MB,)),
            dma((MB,)),
            dma((8,)),
            dma((16,)),
            dma((2,)),
            dma((2 * MB,)),
            pltpu.SemaphoreType.REGULAR,
        ],
        compiler_params=pltpu.CompilerParams(
            collective_id=0, has_side_effects=True, vmem_limit_bytes=60 << 20
        ),
        name="blocks",
    )(qkv_t, out_t, mod_own, states, shifts)


def packed_modulation(mod_part):
    pieces = mod_part.astype(jnp.float32).reshape(MB * 9, 32)
    return jnp.pad(jnp.tile(pieces, (1, 4)), ((0, 6), (0, 0)))


def per_device(states, timesteps, shifts, qkv_weight, out_weight, mod_weight):
    embedding = jax.nn.silu(sinusoid(timesteps, TEMB)).astype(jnp.bfloat16)
    mod_part = jnp.dot(embedding, mod_weight[0], preferred_element_type=jnp.float32).astype(
        jnp.bfloat16
    )
    results = blocks(
        qkv_weight[0].T, out_weight[0].T, packed_modulation(mod_part), states.reshape(MB, 256, D), shifts
    )
    return results.reshape((1,) + states.shape)


def solution(mesh):
    in_specs = (
        P(None, "wrow", "wcol", None),
        P(),
        P("section", None),
        P("section", None, "wcol"),
        P("section", None, "wcol"),
        P("section", None, "wcol"),
    )
    out_specs = P("section", None, "wrow", "wcol", None)
    return jax.shard_map(
        per_device, mesh=mesh, in_specs=in_specs, out_specs=out_specs, check_vma=False
    )
```

```python
import math

import jax
import jax.numpy as jnp
from jax import lax
from jax.experimental import pallas as pl
from jax.experimental.pallas import tpu as pltpu
from jax.sharding import PartitionSpec as P

HEADS = 6
HD = 128
TEMB = 256
MB = 2
D = 1536
MESH = pl.DeviceIdType.MESH
UNIT = 48
EPSILON = 1e-06
BF16 = jnp.bfloat16
F32 = jnp.float32


def sinusoid(moments, entries):
    half_count = entries // 2
    frequency = jnp.exp(-math.log(10000.0) * jnp.arange(half_count, dtype=jnp.float32) / half_count)
    angles = moments.astype(jnp.float32)[:, None] * frequency[None, :]
    return jnp.concatenate([jnp.cos(angles), jnp.sin(angles)], axis=1)


def unit_row(w, q):
    last = q // 3
    return (144 * w + UNIT * q) * (1 - last) + (2304 + UNIT * w) * last


ORDER = (
    (0, -1), (0, 1), (-1, 0), (1, 0), (0, 2), (-1, -1), (1, -1), (-1, 1), (1, 1),
    (-1, 2), (1, 2), (2, 0), (2, -1), (2, 1), (2, 2),
)


def place():
    row, col = lax.axis_index("wrow"), lax.axis_index("wcol")
    return row, col, row // 2, row % 2, col // 4, col % 4


def gather_weights(qkv_t, out_t, weights, sem_own, sem_send, sem_piece, sem_unit):
    row, col, y, core, x, z = place()
    q = (y % 2) * 2 + core
    qy = ((y + 1) % 2) * 2 + core
    sends = []

    def number(dx, dz):
        return ((x + dx + 4) % 4) * 4 + (z + dz + 4) % 4

    def at_col(dx, dz):
        return {"wcol": number(dx, dz)}

    crossing = [d for d in ORDER if d not in ((-1, 0), (1, 0))]

    def to_row(d):
        up = crossing.index(d) % 2
        return {"wrow": ((y + 7 + 2 * up) % 8) * 2 + core}

    partner = {"wrow": y * 2 + 1 - core}

    def copy(w, quarter, target, slot, piece=None):
        first = 0 if piece is None else 16 * piece
        count = UNIT if piece is None else 16
        part = weights.at[pl.ds(pl.multiple_of(unit_row(w, quarter) + first, 16), count), :]
        return pltpu.make_async_remote_copy(
            src_ref=part,
            dst_ref=part,
            send_sem=sem_send.at[slot],
            recv_sem=sem_unit.at[w * 4 + quarter] if piece is None else sem_piece.at[w * 3 + piece],
            device_id=target,
            device_id_type=MESH,
        )

    def send(w, quarter, target, piece=None):
        c = copy(w, quarter, target, len(sends), piece)
        c.start()
        sends.append(c)

    def arrived(w, quarter, piece=None):
        copy(w, quarter, partner, 0, piece).wait_recv()

    def unit(w, quarter):
        return weights.at[pl.ds(pl.multiple_of(unit_row(w, quarter), 16), UNIT), :]

    own = [
        pltpu.make_async_copy(qkv_t.at[pl.ds(UNIT * k, UNIT), :], unit(col, k), sem_own.at[k])
        for k in range(3)
    ] + [
        pltpu.make_async_copy(
            out_t.at[pl.ds(UNIT * k, UNIT), :], unit(col, 3).at[:, pl.ds(768 * k, 768)],
            sem_own.at[3 + k],
        )
        for k in range(2)
    ]

    def load():
        for c in own:
            c.start()
        for c in own:
            c.wait()

    def begin():
        for piece in range(3):
            for d in ((0, 1), (0, -1), (1, 0), (-1, 0)):
                send(col, q, at_col(*d), piece)
        for d in ((1, 0), (-1, 0)):
            send(col, qy, at_col(*d))

    def plane(after_z):
        def event(dx, dz, piece):
            w = number(dx, dz)
            arrived(w, q, piece)
            if dz == -1 and dx == 0 and piece < 2:
                send(w, q, at_col(0, 1), piece)
            if dz == 1 and dx == 0 and piece == 2:
                send(w, q, at_col(0, -1), piece)
            if dx == 0:
                send(w, q, at_col(1, 0), piece)
                send(w, q, at_col(-1, 0), piece)
            if dx == -1 and dz in (0, -1):
                send(w, q, at_col(1, 0), piece)
            if dx == 1 and dz in (1, 2):
                send(w, q, at_col(-1, 0), piece)

        def whole(dx, dz):
            w = number(dx, dz)
            if (dx, dz) in crossing:
                send(w, q, to_row((dx, dz)))
            send(w, q, partner)

        for group in (((0, -1), (0, 1), (-1, 0), (1, 0)), ((0, 2),)):
            for piece in range(3):
                for d in group:
                    event(*d, piece)
            for d in group:
                whole(*d)
        after_z()
        for d in ORDER[5:]:
            for piece in range(3):
                event(*d, piece)
            whole(*d)

    def rows():
        for d in ((-1, 0), (1, 0), (0, -1), (0, 1)) + ORDER[4:]:
            arrived(number(*d), qy)
            send(number(*d), qy, partner)

    def sides():
        for d in ORDER:
            arrived(number(*d), (y % 2) * 2 + 1 - core)
        for d in ORDER:
            arrived(number(*d), ((y + 1) % 2) * 2 + 1 - core)

    def finish():
        for c in sends:
            c.wait_send()

    return load, begin, plane, rows, sides, finish


def iota(shape, axis):
    return lax.broadcasted_iota(jnp.int32, shape, axis)


def one_hot(index, width):
    return jnp.where(iota((index.shape[0], width), 1) == index, 1.0, 0.0).astype(BF16)


def pick(selector, rows):
    return jnp.dot(selector, rows, preferred_element_type=F32)


def times_rows(left, right):
    return lax.dot_general(left, right, (((1,), (1,)), ((), ())), preferred_element_type=F32)


def cell_slot(i, j):
    return jnp.where(j < 16, 16 * i + j, 304 + 4 * i + j)


def window_slot(u, v):
    slot = ((u >> 3) * 2 + (v >> 3)) * 64 + (u & 7) * 8 + (v & 7)
    inside = (u >= 0) & (u < 16) & (v >= 0) & (v < 16)
    return jnp.where(inside, slot, -1)


def block_kernel(
    qkv_t, out_t, mod_own, states, shifts, out_ref,
    weights, out_rows, first_packed, first_rows, mods, modv, gates, first_gates,
    ext, pack, spread_in, spread_back, spread_own, spread_rim,
    rolled, normed, triples, att, rim, back, handed, result,
    sem_own, sem_send, sem_piece, sem_unit, sem_ms, sem_mr,
    sem_x, sem_hs, sem_hr, sem_bs, sem_br, sem_ps, sem_pr, sem_o, sem_fs, sem_fr, sem_gs,
    sem_cs, sem_go,
):
    row, col, y, core, x, z = place()
    section = lax.axis_index("section")
    load, begin, plane, rows, sides, finish = gather_weights(
        qkv_t, out_t, weights, sem_own, sem_send, sem_piece, sem_unit
    )
    row_up, row_down = (row + 1) % 16, (row + 15) % 16
    col_up, col_down = (col + 1) % 16, (col + 15) % 16

    barrier = pltpu.get_barrier_semaphore()
    peers = [{"wcol": (col + k) % 16} for k in range(1, 16)]
    near = [
        {"wrow": y * 2 + 1 - core},
        {"wrow": ((y + 1) % 8) * 2 + core},
        {"wrow": ((y + 7) % 8) * 2 + core},
        {"wrow": (row + 2 * core + 15) % 16},
        {"wrow": row_up, "wcol": col_up},
        {"wrow": row_down, "wcol": col_down},
        {"section": 1 - section},
        {"section": 1 - section, "wcol": (col + 15 + 2 * section) % 16},
        {
            "section": 1 - section,
            "wrow": (row + 15 + 2 * section) % 16,
            "wcol": (col + 15 + 2 * section) % 16,
        },
    ]
    for peer in peers + near:
        pl.semaphore_signal(barrier, inc=1, device_id=peer, device_id_type=MESH)
    load()
    pl.semaphore_wait(barrier, len(peers) + len(near))

    def remote(source, target, send_sem, recv_sem, device):
        return pltpu.make_async_remote_copy(
            src_ref=source,
            dst_ref=target,
            send_sem=send_sem,
            recv_sem=recv_sem,
            device_id=device,
            device_id_type=MESH,
        )

    def own_state(b, target):
        return pltpu.make_async_copy(states.at[b], target, sem_x.at[b])

    def hand_over(b):
        return remote(
            handed.at[b], handed.at[b], sem_ps.at[b], sem_pr.at[b], {"section": 1 - section}
        )

    def hand_gates():
        return remote(gates, first_gates, sem_gs.at[0], sem_gs.at[1], {"section": 1 - section})

    def first_unit(slot, w, device):
        part = pl.ds(pl.multiple_of(UNIT * w, 16), UNIT)
        return remote(
            weights.at[pl.ds(pl.multiple_of(2304 + UNIT * w, 16), UNIT), :],
            first_packed.at[part, :], sem_fs.at[slot], sem_fr.at[w], device,
        )

    def relay_unit(slot, w, device):
        part = pl.ds(pl.multiple_of(UNIT * w, 16), UNIT)
        return remote(
            first_packed.at[part, :], first_packed.at[part, :], sem_fs.at[slot], sem_fr.at[w],
            device,
        )

    def first_own(k):
        return 4 * k + 2 * core + y % 2

    def first_near(k):
        return 4 * k + 2 * core + (y + 1) % 2

    behind = {"section": 1 - section, "wcol": col_down}
    partner = {"wrow": y * 2 + 1 - core}

    def first_sends():
        return [first_unit(k, first_own(k), behind) for k in range(4)]

    def first_rows_sends():
        return [
            relay_unit(k, first_own(k), {"wrow": ((y + (1 if k < 2 else 7)) % 8) * 2 + core})
            for k in range(4)
        ]

    def first_relays():
        return [relay_unit(4 + k, first_own(k), partner) for k in range(4)] + [
            relay_unit(8 + k, first_near(k), partner) for k in range(4)
        ]

    def receive_first():
        swaps, relays = first_rows_sends(), first_relays()
        for k in range(4):
            first_unit(k, first_own(k), behind).wait_recv()
            swaps[k].start()
            relays[k].start()
        for k in range(4):
            first_unit(k, first_near(k), behind).wait_recv()
            relays[4 + k].start()
        for k in range(4):
            for cls in range(2):
                first_unit(k, 4 * k + 2 * (1 - core) + cls, behind).wait_recv()
        unpack(first_packed, 0, first_rows)

    def borders(b):
        def piece(k, source, first, count, device):
            return remote(
                source, ext.at[b, pl.ds(first, count), :], sem_hs.at[3 * b + k],
                sem_hr.at[3 * b + k], device,
            )

        return (
            piece(0, ext.at[b, pl.ds(0, 64), :], 256, 64, {"wrow": row_down}),
            piece(1, pack.at[b], 320, 64, {"wcol": col_down}),
            piece(2, pack.at[b, pl.ds(0, 16), :], 384, 16, {"wrow": row_down, "wcol": col_down}),
        )

    def returns(b):
        def piece(k, at, count, device):
            part = pl.ds(at, count)
            return remote(
                back.at[b, part, :], rim.at[b, part, :],
                sem_bs.at[3 * b + k], sem_br.at[3 * b + k], device,
            )

        return (
            piece(0, 0, 64, {"wrow": row_up}),
            piece(1, 64, 64, {"wcol": col_up}),
            piece(2, 128, 16, {"wrow": row_up, "wcol": col_up}),
        )

    def cross_borders(b):
        def piece(k, count, device):
            return remote(
                pack.at[b, pl.ds(0, count), :], ext.at[b, pl.ds(256 + 64 * k, count), :],
                sem_cs.at[2 * b + k - 1], sem_hr.at[3 * b + k], device,
            )

        return (
            piece(1, 64, {"section": 1 - section, "wcol": col_down}),
            piece(2, 16, {"section": 1 - section, "wrow": row_down, "wcol": col_down}),
        )

    def pack_columns(b, source):
        t = iota((64, 1), 0)
        selector = one_hot((t >> 2) * 16 + (t & 3), 256)
        pack[b] = pick(selector, source).astype(BF16)

    @pl.when(section == 0)
    def _():
        for b in range(MB):
            own_state(b, ext.at[b, pl.ds(0, 256), :]).start()

    @pl.when(section == 1)
    def _():
        for b in range(MB):
            own_state(b, result.at[b]).start()

    def go():
        pl.semaphore_signal(
            sem_go, inc=1, device_id={"section": 1 - section}, device_id_type=MESH
        )

    @pl.when(section == 1)
    def _():
        pl.semaphore_wait(sem_go, 1)

    begin()

    mods[pl.ds(col, 1)] = mod_own[...][None]
    msends = [
        remote(mod_own, mods.at[col], sem_ms.at[k], sem_mr.at[col], peers[k - 1])
        for k in range(1, 16)
    ]

    for b in range(MB):
        ext[b, 400:512, :] = jnp.zeros((112, D), BF16)
        rim[b, 144:256, :] = jnp.zeros((112, HEADS * HD), BF16)

    r, c = shifts[0, 0], shifts[0, 1]
    t = iota((256, 1), 0)
    i = r + 8 * (t >> 7) + ((t >> 3) & 7)
    j = c + 8 * ((t >> 6) & 1) + (t & 7)
    spread_in[...] = one_hot(cell_slot(i, j), 512)
    i, j = t >> 4, t & 15
    spread_own[...] = one_hot(window_slot(i - r, j - c), 256)
    index = jnp.where(
        i >= r,
        jnp.where(j >= c, -1, 64 + 4 * i + j),
        jnp.where(j >= c, 16 * i + j, 128 + 4 * i + j),
    )
    spread_rim[...] = one_hot(index, 256)
    t = iota((144, 1), 0)
    s = t - 64
    q = t - 128
    i = jnp.where(t < 64, 16 + (t >> 4), jnp.where(t < 128, s >> 2, 16 + (q >> 2)))
    j = jnp.where(t < 64, t & 15, 16 + (t & 3))
    spread_back[...] = one_hot(window_slot(i - r, j - c), 256)

    def after_z():
        for copy in msends:
            copy.start()

        @pl.when(section == 0)
        def _():
            go()
            for b in range(MB):
                own_state(b, ext.at[b, pl.ds(0, 256), :]).wait()
                pack_columns(b, ext[b, 0:256, :])
                for copy in borders(b):
                    copy.start()

    plane(after_z)
    rows()
    for k in range(1, 16):
        other = (col + k) % 16
        remote(mod_own, mods.at[other], sem_ms.at[k], sem_mr.at[other], peers[k - 1]).wait_recv()

    pieces = mods[...].reshape(256, 128)
    turned = jnp.concatenate([pieces[:, 64:], pieces[:, :64]], axis=1)
    low = iota((256, 128), 1) < 64
    lane = iota((40, 128), 1) >> 5
    gates[...] = jnp.zeros((8, D), F32)
    for b in range(MB):
        joined = jnp.zeros((40, 128), F32)
        whole = jnp.where(low, pieces, turned) if b == 0 else jnp.where(low, turned, pieces)
        for k in range(4):
            piece = iota((40, 1), 0) * 4 + k
            shard = (piece * 57) >> 9
            index = jnp.where(piece < 144, 16 * shard + piece - 9 * shard, -1)
            joined = jnp.where(lane == k, pick(one_hot(index, 256), whole), joined)
        for t in range(24):
            modv[b, :, 128 * t : 128 * t + 128] = jnp.broadcast_to(joined[t : t + 1], (8, 128))
        for t in range(12):
            gates[b : b + 1, 128 * t : 128 * t + 128] = joined[24 + t : 25 + t]

    def unpack(source, base, target):
        for w in range(16):
            packed = source[base + UNIT * w : base + UNIT * w + UNIT, :]
            target[96 * w : 96 * w + 48, :] = packed[:, :768]
            target[96 * w + 48 : 96 * w + 96, :] = packed[:, 768:]

    def add_projection(source, matrix, gate, kept, target):
        for k in range(6):
            here = slice(256 * k, 256 * k + 256)
            projection = times_rows(source, matrix[here, :]).astype(BF16)
            target[:, here] = (
                kept[:, here].astype(F32) + gate[:, here] * projection.astype(F32)
            ).astype(BF16)

    def prepare(b):
        for copy in borders(b):
            copy.wait_recv()
        for k in range(3):
            here = slice(512 * k, 512 * k + 512)
            rolled[:, here] = pick(spread_in[...], ext[b, :, here]).astype(BF16)
        scale = 1.0 + modv[b, 0:1, D : 2 * D]
        shift = modv[b, 0:1, 0:D]
        for k in range(8):
            here = slice(32 * k, 32 * k + 32)
            values = rolled[here, :].astype(F32)
            center = values - jnp.mean(values, axis=-1, keepdims=True)
            spread = jnp.mean(center * center, axis=-1, keepdims=True)
            center = center * lax.rsqrt(spread + EPSILON)
            normed[b, here, :] = (center * scale + shift).astype(BF16)
    def compute(b):
        for k in range(3):
            here = slice(768 * k, 768 * k + 768)
            triples[here, :] = times_rows(weights[here, :], normed[b]).astype(BF16)

        same = (iota((128, 128), 0) >> 6) == (iota((128, 128), 1) >> 6)
        for head in range(HEADS):
            for pair in range(2):
                here = slice(128 * pair, 128 * pair + 128)
                query, key, value = (
                    triples[768 * n + HD * head : 768 * n + HD * head + HD, here] for n in range(3)
                )
                scores = lax.dot_general(
                    key, query, (((0,), (0,)), ((), ())), preferred_element_type=F32
                ) * HD ** (-0.5)
                powers = jnp.where(same, jnp.exp(jnp.where(same, scores, 0.0)), 0.0)
                total = jnp.sum(powers, axis=0, keepdims=True)
                chances = (powers / total).astype(BF16)
                att[b, HD * head : HD * head + HD, here] = pick(value, chances).astype(BF16)

        back[b] = times_rows(spread_back[...], att[b]).astype(BF16)
        for copy in returns(b):
            copy.start()

    def restore(b):
        for copy in returns(b):
            copy.wait_recv()
        own = times_rows(spread_own[...], att[b])
        handed[b] = (own + pick(spread_rim[...], rim[b])).astype(BF16)

        @pl.when(section == 0)
        def _():
            hand_over(b).start()

    def project(b):
        add_projection(
            handed[b], out_rows, gates[b : b + 1, :], ext.at[b, pl.ds(0, 256), :], result.at[b]
        )

        @pl.when(section == 0)
        def _():
            for copy in borders(b)[1:]:
                copy.wait_send()
            pack_columns(b, result[b])
            for copy in cross_borders(b):
                copy.start()

        pltpu.make_async_copy(result.at[b], out_ref.at[b], sem_o.at[b]).start()

    @pl.when(section == 0)
    def _():
        for b in range(MB):
            prepare(b)

    sides()

    @pl.when(section == 0)
    def _():
        hand_gates().start()
        for copy in first_sends():
            copy.start()

    def next_state(b):
        own_state(b, result.at[b]).wait()
        hand_over(b).wait_recv()
        add_projection(
            handed[b], first_rows, first_gates[b : b + 1, :], result.at[b],
            ext.at[b, pl.ds(0, 256), :],
        )
        borders(b)[0].start()

    @pl.when(section == 0)
    def _():
        compute(0)
        compute(1)
        restore(0)
        unpack(weights, 2304, out_rows)
        project(0)
        restore(1)
        project(1)

    @pl.when(section == 1)
    def _():
        receive_first()
        unpack(weights, 2304, out_rows)
        hand_gates().wait_recv()
        next_state(0)
        prepare(0)
        compute(0)
        next_state(1)
        restore(0)
        project(0)
        prepare(1)
        compute(1)
        restore(1)
        project(1)

    for b in range(MB):
        borders(b)[0].wait_send()
        for copy in returns(b):
            copy.wait_send()
        pltpu.make_async_copy(result.at[b], out_ref.at[b], sem_o.at[b]).wait()

    @pl.when(section == 0)
    def _():
        for b in range(MB):
            hand_over(b).wait_send()
            for copy in cross_borders(b):
                copy.wait_send()
        hand_gates().wait_send()
        for copy in first_sends():
            copy.wait_send()

    @pl.when(section == 1)
    def _():
        for copy in first_rows_sends() + first_relays():
            copy.wait_send()

    finish()
    for copy in msends:
        copy.wait_send()


def blocks(qkv_t, out_t, mod_own, states, shifts):
    dma = pltpu.SemaphoreType.DMA
    return pl.pallas_call(
        block_kernel,
        out_shape=jax.ShapeDtypeStruct((MB, 256, D), BF16),
        in_specs=[
            pl.BlockSpec(memory_space=pl.ANY),
            pl.BlockSpec(memory_space=pl.ANY),
            pl.BlockSpec(memory_space=pltpu.VMEM),
            pl.BlockSpec(memory_space=pl.ANY),
            pl.BlockSpec(memory_space=pltpu.SMEM),
        ],
        out_specs=pl.BlockSpec(memory_space=pl.ANY),
        scratch_shapes=[
            pltpu.VMEM((3072, D), BF16),
            pltpu.VMEM((D, 768), BF16),
            pltpu.VMEM((768, D), BF16),
            pltpu.VMEM((D, 768), BF16),
            pltpu.VMEM((16, 16, 128), BF16),
            pltpu.VMEM((MB, 8, 2 * D), F32),
            pltpu.VMEM((8, D), F32),
            pltpu.VMEM((8, D), F32),
            pltpu.VMEM((MB, 512, D), BF16),
            pltpu.VMEM((MB, 64, D), BF16),
            pltpu.VMEM((256, 512), BF16),
            pltpu.VMEM((144, 256), BF16),
            pltpu.VMEM((256, 256), BF16),
            pltpu.VMEM((256, 256), BF16),
            pltpu.VMEM((256, D), BF16),
            pltpu.VMEM((MB, 256, D), BF16),
            pltpu.VMEM((2304, 256), BF16),
            pltpu.VMEM((MB, 768, 256), BF16),
            pltpu.VMEM((MB, 256, 768), BF16),
            pltpu.VMEM((MB, 144, 768), BF16),
            pltpu.VMEM((MB, 256, 768), BF16),
            pltpu.VMEM((MB, 256, D), BF16),
            dma((5,)),
            dma((96,)),
            dma((48,)),
            dma((64,)),
            dma((16,)),
            dma((16,)),
            dma((MB,)),
            dma((3 * MB,)),
            dma((3 * MB,)),
            dma((3 * MB,)),
            dma((3 * MB,)),
            dma((MB,)),
            dma((MB,)),
            dma((MB,)),
            dma((12,)),
            dma((16,)),
            dma((2,)),
            dma((2 * MB,)),
            pltpu.SemaphoreType.REGULAR,
        ],
        compiler_params=pltpu.CompilerParams(
            collective_id=0, has_side_effects=True, vmem_limit_bytes=60 << 20
        ),
        name="blocks",
    )(qkv_t, out_t, mod_own, states, shifts)


def packed_modulation(mod_part):
    pieces = mod_part.reshape(MB, 9, 1, 32)
    doubled = jnp.concatenate([pieces, pieces], axis=2).transpose(1, 0, 2, 3)
    return jnp.pad(doubled.reshape(9, 128), ((0, 7), (0, 0)))


def per_device(states, timesteps, shifts, qkv_weight, out_weight, mod_weight):
    embedding = jax.nn.silu(sinusoid(timesteps, TEMB)).astype(jnp.bfloat16)
    mod_part = jnp.dot(embedding, mod_weight[0], preferred_element_type=jnp.float32).astype(
        jnp.bfloat16
    )
    results = blocks(
        qkv_weight[0].T, out_weight[0].T, packed_modulation(mod_part), states.reshape(MB, 256, D), shifts
    )
    return results.reshape((1,) + states.shape)


def solution(mesh):
    in_specs = (
        P(None, "wrow", "wcol", None),
        P(),
        P("section", None),
        P("section", None, "wcol"),
        P("section", None, "wcol"),
        P("section", None, "wcol"),
    )
    out_specs = P("section", None, "wrow", "wcol", None)
    return jax.shard_map(
        per_device, mesh=mesh, in_specs=in_specs, out_specs=out_specs, check_vma=False
    )
```

```python
import math

import jax
import jax.numpy as jnp
from jax import lax
from jax.experimental import pallas as pl
from jax.experimental.pallas import tpu as pltpu
from jax.sharding import PartitionSpec as P

HEADS = 6
HD = 128
TEMB = 256
MB = 2
D = 1536
MESH = pl.DeviceIdType.MESH
UNIT = 48
EPSILON = 1e-06
BF16 = jnp.bfloat16
F32 = jnp.float32


def sinusoid(moments, entries):
    half_count = entries // 2
    frequency = jnp.exp(-math.log(10000.0) * jnp.arange(half_count, dtype=jnp.float32) / half_count)
    angles = moments.astype(jnp.float32)[:, None] * frequency[None, :]
    return jnp.concatenate([jnp.cos(angles), jnp.sin(angles)], axis=1)


def unit_row(w, q):
    last = q // 3
    return (144 * w + UNIT * q) * (1 - last) + (2304 + UNIT * w) * last


ORDER = (
    (0, -1), (0, 1), (-1, 0), (1, 0), (0, 2), (-1, -1), (1, -1), (-1, 1), (1, 1),
    (-1, 2), (1, 2), (2, 0), (2, -1), (2, 1), (2, 2),
)


def place():
    row, col = lax.axis_index("wrow"), lax.axis_index("wcol")
    return row, col, row // 2, row % 2, col // 4, col % 4


def gather_weights(qkv_t, out_t, weights, sem_own, sem_send, sem_piece, sem_unit):
    row, col, y, core, x, z = place()
    q = (y % 2) * 2 + core
    qy = ((y + 1) % 2) * 2 + core
    sends = []

    def number(dx, dz):
        return ((x + dx + 4) % 4) * 4 + (z + dz + 4) % 4

    def at_col(dx, dz):
        return {"wcol": number(dx, dz)}

    crossing = [d for d in ORDER if d not in ((-1, 0), (1, 0))]

    def to_row(d):
        up = crossing.index(d) % 2
        return {"wrow": ((y + 7 + 2 * up) % 8) * 2 + core}

    partner = {"wrow": y * 2 + 1 - core}

    def copy(w, quarter, target, slot, piece=None):
        first = 0 if piece is None else 16 * piece
        count = UNIT if piece is None else 16
        part = weights.at[pl.ds(pl.multiple_of(unit_row(w, quarter) + first, 16), count), :]
        return pltpu.make_async_remote_copy(
            src_ref=part,
            dst_ref=part,
            send_sem=sem_send.at[slot],
            recv_sem=sem_unit.at[w * 4 + quarter] if piece is None else sem_piece.at[w * 3 + piece],
            device_id=target,
            device_id_type=MESH,
        )

    def send(w, quarter, target, piece=None):
        c = copy(w, quarter, target, len(sends), piece)
        c.start()
        sends.append(c)

    def arrived(w, quarter, piece=None):
        copy(w, quarter, partner, 0, piece).wait_recv()

    def unit(w, quarter):
        return weights.at[pl.ds(pl.multiple_of(unit_row(w, quarter), 16), UNIT), :]

    own = [
        pltpu.make_async_copy(qkv_t.at[pl.ds(UNIT * k, UNIT), :], unit(col, k), sem_own.at[k])
        for k in range(3)
    ] + [
        pltpu.make_async_copy(
            out_t.at[pl.ds(UNIT * k, UNIT), :], unit(col, 3).at[:, pl.ds(768 * k, 768)],
            sem_own.at[3 + k],
        )
        for k in range(2)
    ]

    def load():
        for c in own:
            c.start()
        for c in own:
            c.wait()

    def begin():
        for piece in range(3):
            for d in ((0, 1), (0, -1), (1, 0), (-1, 0)):
                send(col, q, at_col(*d), piece)
        for d in ((1, 0), (-1, 0)):
            send(col, qy, at_col(*d))

    def plane(after_z):
        def event(dx, dz, piece):
            w = number(dx, dz)
            arrived(w, q, piece)
            if dz == -1 and dx == 0 and piece < 2:
                send(w, q, at_col(0, 1), piece)
            if dz == 1 and dx == 0 and piece == 2:
                send(w, q, at_col(0, -1), piece)
            if dx == 0:
                send(w, q, at_col(1, 0), piece)
                send(w, q, at_col(-1, 0), piece)
            if dx == -1 and dz in (0, -1):
                send(w, q, at_col(1, 0), piece)
            if dx == 1 and dz in (1, 2):
                send(w, q, at_col(-1, 0), piece)

        def whole(dx, dz):
            w = number(dx, dz)
            if (dx, dz) in crossing:
                send(w, q, to_row((dx, dz)))
            send(w, q, partner)

        for group in (((0, -1), (0, 1), (-1, 0), (1, 0)), ((0, 2),)):
            for piece in range(3):
                for d in group:
                    event(*d, piece)
            for d in group:
                whole(*d)
        after_z()
        for d in ORDER[5:]:
            for piece in range(3):
                event(*d, piece)
            whole(*d)

    def rows():
        for d in ((-1, 0), (1, 0), (0, -1), (0, 1)) + ORDER[4:]:
            arrived(number(*d), qy)
            send(number(*d), qy, partner)

    def sides():
        for d in ORDER:
            arrived(number(*d), (y % 2) * 2 + 1 - core)
        for d in ORDER:
            arrived(number(*d), ((y + 1) % 2) * 2 + 1 - core)

    def finish():
        for c in sends:
            c.wait_send()

    return load, begin, plane, rows, sides, finish


def iota(shape, axis):
    return lax.broadcasted_iota(jnp.int32, shape, axis)


def one_hot(index, width):
    return jnp.where(iota((index.shape[0], width), 1) == index, 1.0, 0.0).astype(BF16)


def pick(selector, rows):
    return jnp.dot(selector, rows, preferred_element_type=F32)


def times_rows(left, right):
    return lax.dot_general(left, right, (((1,), (1,)), ((), ())), preferred_element_type=F32)


def cell_slot(i, j):
    return jnp.where(j < 16, 16 * i + j, 304 + 4 * i + j)


def window_slot(u, v):
    slot = ((u >> 3) * 2 + (v >> 3)) * 64 + (u & 7) * 8 + (v & 7)
    inside = (u >= 0) & (u < 16) & (v >= 0) & (v < 16)
    return jnp.where(inside, slot, -1)


def block_kernel(
    qkv_t, out_t, mod_own, states, shifts, out_ref,
    weights, out_rows, first_packed, first_rows, mods, modv, gates, first_gates,
    ext, pack, spread_in, spread_back, spread_own, spread_rim,
    rolled, normed, triples, att, rim, back, handed, result,
    sem_own, sem_send, sem_piece, sem_unit, sem_ms, sem_mr,
    sem_x, sem_hs, sem_hr, sem_bs, sem_br, sem_ps, sem_pr, sem_o, sem_fs, sem_fr, sem_gs,
    sem_cs,
):
    row, col, y, core, x, z = place()
    section = lax.axis_index("section")
    load, begin, plane, rows, sides, finish = gather_weights(
        qkv_t, out_t, weights, sem_own, sem_send, sem_piece, sem_unit
    )
    row_up, row_down = (row + 1) % 16, (row + 15) % 16
    col_up, col_down = (col + 1) % 16, (col + 15) % 16

    barrier = pltpu.get_barrier_semaphore()
    peers = [{"wcol": (col + k) % 16} for k in range(1, 16)]
    near = [
        {"wrow": y * 2 + 1 - core},
        {"wrow": ((y + 1) % 8) * 2 + core},
        {"wrow": ((y + 7) % 8) * 2 + core},
        {"wrow": (row + 2 * core + 15) % 16},
        {"wrow": row_up, "wcol": col_up},
        {"wrow": row_down, "wcol": col_down},
        {"section": 1 - section},
        {"section": 1 - section, "wcol": (col + 15 + 2 * section) % 16},
        {
            "section": 1 - section,
            "wrow": (row + 15 + 2 * section) % 16,
            "wcol": (col + 15 + 2 * section) % 16,
        },
    ]
    for peer in peers + near:
        pl.semaphore_signal(barrier, inc=1, device_id=peer, device_id_type=MESH)
    load()
    pl.semaphore_wait(barrier, len(peers) + len(near))

    def remote(source, target, send_sem, recv_sem, device):
        return pltpu.make_async_remote_copy(
            src_ref=source,
            dst_ref=target,
            send_sem=send_sem,
            recv_sem=recv_sem,
            device_id=device,
            device_id_type=MESH,
        )

    def own_state(b, target):
        return pltpu.make_async_copy(states.at[b], target, sem_x.at[b])

    def hand_over(b):
        return remote(
            handed.at[b], handed.at[b], sem_ps.at[b], sem_pr.at[b], {"section": 1 - section}
        )

    def hand_gates():
        return remote(gates, first_gates, sem_gs.at[0], sem_gs.at[1], {"section": 1 - section})

    def first_unit(slot, w, device):
        part = pl.ds(pl.multiple_of(UNIT * w, 16), UNIT)
        return remote(
            weights.at[pl.ds(pl.multiple_of(2304 + UNIT * w, 16), UNIT), :],
            first_packed.at[part, :], sem_fs.at[slot], sem_fr.at[w], device,
        )

    def relay_unit(slot, w, device):
        part = pl.ds(pl.multiple_of(UNIT * w, 16), UNIT)
        return remote(
            first_packed.at[part, :], first_packed.at[part, :], sem_fs.at[slot], sem_fr.at[w],
            device,
        )

    def first_own(k):
        return 4 * k + 2 * core + y % 2

    def first_near(k):
        return 4 * k + 2 * core + (y + 1) % 2

    behind = {"section": 1 - section, "wcol": col_down}
    partner = {"wrow": y * 2 + 1 - core}

    def first_sends():
        return [first_unit(k, first_own(k), behind) for k in range(4)]

    def first_rows_sends():
        return [
            relay_unit(k, first_own(k), {"wrow": ((y + (1 if k < 2 else 7)) % 8) * 2 + core})
            for k in range(4)
        ]

    def first_relays():
        return [relay_unit(4 + k, first_own(k), partner) for k in range(4)] + [
            relay_unit(8 + k, first_near(k), partner) for k in range(4)
        ]

    def receive_first():
        swaps, relays = first_rows_sends(), first_relays()
        for k in range(4):
            first_unit(k, first_own(k), behind).wait_recv()
            swaps[k].start()
            relays[k].start()
        for k in range(4):
            first_unit(k, first_near(k), behind).wait_recv()
            relays[4 + k].start()
        for k in range(4):
            for cls in range(2):
                first_unit(k, 4 * k + 2 * (1 - core) + cls, behind).wait_recv()
        unpack(first_packed, 0, first_rows)

    def borders(b):
        def piece(k, source, first, count, device):
            return remote(
                source, ext.at[b, pl.ds(first, count), :], sem_hs.at[3 * b + k],
                sem_hr.at[3 * b + k], device,
            )

        return (
            piece(0, ext.at[b, pl.ds(0, 64), :], 256, 64, {"wrow": row_down}),
            piece(1, pack.at[b], 320, 64, {"wcol": col_down}),
            piece(2, pack.at[b, pl.ds(0, 16), :], 384, 16, {"wrow": row_down, "wcol": col_down}),
        )

    def returns(b):
        def piece(k, at, count, device):
            part = pl.ds(at, count)
            return remote(
                back.at[b, part, :], rim.at[b, part, :],
                sem_bs.at[3 * b + k], sem_br.at[3 * b + k], device,
            )

        return (
            piece(0, 0, 64, {"wrow": row_up}),
            piece(1, 64, 64, {"wcol": col_up}),
            piece(2, 128, 16, {"wrow": row_up, "wcol": col_up}),
        )

    def cross_borders(b):
        def piece(k, count, device):
            return remote(
                pack.at[b, pl.ds(0, count), :], ext.at[b, pl.ds(256 + 64 * k, count), :],
                sem_cs.at[2 * b + k - 1], sem_hr.at[3 * b + k], device,
            )

        return (
            piece(1, 64, {"section": 1 - section, "wcol": col_down}),
            piece(2, 16, {"section": 1 - section, "wrow": row_down, "wcol": col_down}),
        )

    def pack_columns(b, source):
        t = iota((64, 1), 0)
        selector = one_hot((t >> 2) * 16 + (t & 3), 256)
        pack[b] = pick(selector, source).astype(BF16)

    @pl.when(section == 0)
    def _():
        for b in range(MB):
            own_state(b, ext.at[b, pl.ds(0, 256), :]).start()

    @pl.when(section == 1)
    def _():
        for b in range(MB):
            own_state(b, result.at[b]).start()

    begin()

    mods[pl.ds(col, 1)] = mod_own[...][None]
    msends = [
        remote(mod_own, mods.at[col], sem_ms.at[k], sem_mr.at[col], peers[k - 1])
        for k in range(1, 16)
    ]

    for b in range(MB):
        ext[b, 400:512, :] = jnp.zeros((112, D), BF16)
        rim[b, 144:256, :] = jnp.zeros((112, HEADS * HD), BF16)

    r, c = shifts[0, 0], shifts[0, 1]
    t = iota((256, 1), 0)
    i = r + 8 * (t >> 7) + ((t >> 3) & 7)
    j = c + 8 * ((t >> 6) & 1) + (t & 7)
    spread_in[...] = one_hot(cell_slot(i, j), 512)
    i, j = t >> 4, t & 15
    spread_own[...] = one_hot(window_slot(i - r, j - c), 256)
    index = jnp.where(
        i >= r,
        jnp.where(j >= c, -1, 64 + 4 * i + j),
        jnp.where(j >= c, 16 * i + j, 128 + 4 * i + j),
    )
    spread_rim[...] = one_hot(index, 256)
    t = iota((144, 1), 0)
    s = t - 64
    q = t - 128
    i = jnp.where(t < 64, 16 + (t >> 4), jnp.where(t < 128, s >> 2, 16 + (q >> 2)))
    j = jnp.where(t < 64, t & 15, 16 + (t & 3))
    spread_back[...] = one_hot(window_slot(i - r, j - c), 256)

    def after_z():
        for copy in msends:
            copy.start()

        @pl.when(section == 0)
        def _():
            for b in range(MB):
                own_state(b, ext.at[b, pl.ds(0, 256), :]).wait()
                pack_columns(b, ext[b, 0:256, :])
                for copy in borders(b):
                    copy.start()

    plane(after_z)
    for k in range(1, 16):
        other = (col + k) % 16
        remote(mod_own, mods.at[other], sem_ms.at[k], sem_mr.at[other], peers[k - 1]).wait_recv()

    pieces = mods[...].reshape(256, 128)
    turned = jnp.concatenate([pieces[:, 64:], pieces[:, :64]], axis=1)
    low = iota((256, 128), 1) < 64
    lane = iota((40, 128), 1) >> 5
    gates[...] = jnp.zeros((8, D), F32)
    for b in range(MB):
        joined = jnp.zeros((40, 128), F32)
        whole = jnp.where(low, pieces, turned) if b == 0 else jnp.where(low, turned, pieces)
        for k in range(4):
            piece = iota((40, 1), 0) * 4 + k
            shard = (piece * 57) >> 9
            index = jnp.where(piece < 144, 16 * shard + piece - 9 * shard, -1)
            joined = jnp.where(lane == k, pick(one_hot(index, 256), whole), joined)
        for t in range(24):
            modv[b, :, 128 * t : 128 * t + 128] = jnp.broadcast_to(joined[t : t + 1], (8, 128))
        for t in range(12):
            gates[b : b + 1, 128 * t : 128 * t + 128] = joined[24 + t : 25 + t]

    def unpack(source, base, target):
        for w in range(16):
            packed = source[base + UNIT * w : base + UNIT * w + UNIT, :]
            target[96 * w : 96 * w + 48, :] = packed[:, :768]
            target[96 * w + 48 : 96 * w + 96, :] = packed[:, 768:]

    def add_projection(source, matrix, gate, kept, target):
        for k in range(6):
            here = slice(256 * k, 256 * k + 256)
            projection = times_rows(source, matrix[here, :]).astype(BF16)
            target[:, here] = (
                kept[:, here].astype(F32) + gate[:, here] * projection.astype(F32)
            ).astype(BF16)

    def prepare(b):
        for copy in borders(b):
            copy.wait_recv()
        for k in range(3):
            here = slice(512 * k, 512 * k + 512)
            rolled[:, here] = pick(spread_in[...], ext[b, :, here]).astype(BF16)
        scale = 1.0 + modv[b, 0:1, D : 2 * D]
        shift = modv[b, 0:1, 0:D]
        for k in range(8):
            here = slice(32 * k, 32 * k + 32)
            values = rolled[here, :].astype(F32)
            center = values - jnp.mean(values, axis=-1, keepdims=True)
            spread = jnp.mean(center * center, axis=-1, keepdims=True)
            center = center * lax.rsqrt(spread + EPSILON)
            normed[b, here, :] = (center * scale + shift).astype(BF16)
    def compute(b):
        for k in range(3):
            here = slice(768 * k, 768 * k + 768)
            triples[here, :] = times_rows(weights[here, :], normed[b]).astype(BF16)

        same = (iota((128, 128), 0) >> 6) == (iota((128, 128), 1) >> 6)
        for head in range(HEADS):
            for pair in range(2):
                here = slice(128 * pair, 128 * pair + 128)
                query, key, value = (
                    triples[768 * n + HD * head : 768 * n + HD * head + HD, here] for n in range(3)
                )
                scores = lax.dot_general(
                    key, query, (((0,), (0,)), ((), ())), preferred_element_type=F32
                ) * HD ** (-0.5)
                powers = jnp.where(same, jnp.exp(jnp.where(same, scores, 0.0)), 0.0)
                total = jnp.sum(powers, axis=0, keepdims=True)
                chances = (powers / total).astype(BF16)
                att[b, HD * head : HD * head + HD, here] = pick(value, chances).astype(BF16)

        back[b] = times_rows(spread_back[...], att[b]).astype(BF16)
        for copy in returns(b):
            copy.start()

    def restore(b):
        for copy in returns(b):
            copy.wait_recv()
        own = times_rows(spread_own[...], att[b])
        handed[b] = (own + pick(spread_rim[...], rim[b])).astype(BF16)

        @pl.when(section == 0)
        def _():
            hand_over(b).start()

    def project(b):
        add_projection(
            handed[b], out_rows, gates[b : b + 1, :], ext.at[b, pl.ds(0, 256), :], result.at[b]
        )

        @pl.when(section == 0)
        def _():
            for copy in borders(b)[1:]:
                copy.wait_send()
            pack_columns(b, result[b])
            for copy in cross_borders(b):
                copy.start()

        pltpu.make_async_copy(result.at[b], out_ref.at[b], sem_o.at[b]).start()

    @pl.when(section == 0)
    def _():
        for b in range(MB):
            prepare(b)

    rows()
    sides()

    @pl.when(section == 0)
    def _():
        hand_gates().start()
        for copy in first_sends():
            copy.start()

    def next_state(b):
        own_state(b, result.at[b]).wait()
        hand_over(b).wait_recv()
        add_projection(
            handed[b], first_rows, first_gates[b : b + 1, :], result.at[b],
            ext.at[b, pl.ds(0, 256), :],
        )
        borders(b)[0].start()

    @pl.when(section == 0)
    def _():
        compute(0)
        compute(1)
        restore(0)
        unpack(weights, 2304, out_rows)
        project(0)
        restore(1)
        project(1)

    @pl.when(section == 1)
    def _():
        receive_first()
        hand_gates().wait_recv()
        next_state(0)
        prepare(0)
        compute(0)
        next_state(1)
        unpack(weights, 2304, out_rows)
        restore(0)
        project(0)
        prepare(1)
        compute(1)
        restore(1)
        project(1)

    for b in range(MB):
        borders(b)[0].wait_send()
        for copy in returns(b):
            copy.wait_send()
        pltpu.make_async_copy(result.at[b], out_ref.at[b], sem_o.at[b]).wait()

    @pl.when(section == 0)
    def _():
        for b in range(MB):
            hand_over(b).wait_send()
            for copy in cross_borders(b):
                copy.wait_send()
        hand_gates().wait_send()
        for copy in first_sends():
            copy.wait_send()

    @pl.when(section == 1)
    def _():
        for copy in first_rows_sends() + first_relays():
            copy.wait_send()

    finish()
    for copy in msends:
        copy.wait_send()


def blocks(qkv_t, out_t, mod_own, states, shifts):
    dma = pltpu.SemaphoreType.DMA
    return pl.pallas_call(
        block_kernel,
        out_shape=jax.ShapeDtypeStruct((MB, 256, D), BF16),
        in_specs=[
            pl.BlockSpec(memory_space=pl.ANY),
            pl.BlockSpec(memory_space=pl.ANY),
            pl.BlockSpec(memory_space=pltpu.VMEM),
            pl.BlockSpec(memory_space=pl.ANY),
            pl.BlockSpec(memory_space=pltpu.SMEM),
        ],
        out_specs=pl.BlockSpec(memory_space=pl.ANY),
        scratch_shapes=[
            pltpu.VMEM((3072, D), BF16),
            pltpu.VMEM((D, 768), BF16),
            pltpu.VMEM((768, D), BF16),
            pltpu.VMEM((D, 768), BF16),
            pltpu.VMEM((16, 16, 128), BF16),
            pltpu.VMEM((MB, 8, 2 * D), F32),
            pltpu.VMEM((8, D), F32),
            pltpu.VMEM((8, D), F32),
            pltpu.VMEM((MB, 512, D), BF16),
            pltpu.VMEM((MB, 64, D), BF16),
            pltpu.VMEM((256, 512), BF16),
            pltpu.VMEM((144, 256), BF16),
            pltpu.VMEM((256, 256), BF16),
            pltpu.VMEM((256, 256), BF16),
            pltpu.VMEM((256, D), BF16),
            pltpu.VMEM((MB, 256, D), BF16),
            pltpu.VMEM((2304, 256), BF16),
            pltpu.VMEM((MB, 768, 256), BF16),
            pltpu.VMEM((MB, 256, 768), BF16),
            pltpu.VMEM((MB, 144, 768), BF16),
            pltpu.VMEM((MB, 256, 768), BF16),
            pltpu.VMEM((MB, 256, D), BF16),
            dma((5,)),
            dma((96,)),
            dma((48,)),
            dma((64,)),
            dma((16,)),
            dma((16,)),
            dma((MB,)),
            dma((3 * MB,)),
            dma((3 * MB,)),
            dma((3 * MB,)),
            dma((3 * MB,)),
            dma((MB,)),
            dma((MB,)),
            dma((MB,)),
            dma((12,)),
            dma((16,)),
            dma((2,)),
            dma((2 * MB,)),
        ],
        compiler_params=pltpu.CompilerParams(
            collective_id=0, has_side_effects=True, vmem_limit_bytes=60 << 20
        ),
        name="blocks",
    )(qkv_t, out_t, mod_own, states, shifts)


def packed_modulation(mod_part):
    pieces = mod_part.reshape(MB, 9, 1, 32)
    doubled = jnp.concatenate([pieces, pieces], axis=2).transpose(1, 0, 2, 3)
    return jnp.pad(doubled.reshape(9, 128), ((0, 7), (0, 0)))


def per_device(states, timesteps, shifts, qkv_weight, out_weight, mod_weight):
    embedding = jax.nn.silu(sinusoid(timesteps, TEMB)).astype(jnp.bfloat16)
    mod_part = jnp.dot(embedding, mod_weight[0], preferred_element_type=jnp.float32).astype(
        jnp.bfloat16
    )
    results = blocks(
        qkv_weight[0].T, out_weight[0].T, packed_modulation(mod_part), states.reshape(MB, 256, D), shifts
    )
    return results.reshape((1,) + states.shape)


def solution(mesh):
    in_specs = (
        P(None, "wrow", "wcol", None),
        P(),
        P("section", None),
        P("section", None, "wcol"),
        P("section", None, "wcol"),
        P("section", None, "wcol"),
    )
    out_specs = P("section", None, "wrow", "wcol", None)
    return jax.shard_map(
        per_device, mesh=mesh, in_specs=in_specs, out_specs=out_specs, check_vma=False
    )
```
